32 devices in a mesh: fsdp: 32 (over z, y, x, core).
Axes of the slice: x: 2, y: 2, z: 4, core: 2. Of those that a mesh axis runs over, the one named last changes fastest.
Arguments:
- tokens: int32 [32, 256], P('fsdp')
- embed_table: float32 [32000, 2048], P('fsdp')
- norm_gain: float32 [2048], P('fsdp')
- w_query: float32 [2048, 2048], P('fsdp')
- w_key: float32 [2048, 2048], P('fsdp')
- w_value: float32 [2048, 2048], P('fsdp')
- d_query: bfloat16 [32, 256, 2048], P('fsdp')
- d_key: bfloat16 [32, 256, 2048], P('fsdp')
- d_value: bfloat16 [32, 256, 2048], P('fsdp')
Outputs:
- output 1: bfloat16 [32, 256, 2048], P('fsdp')
- output 2: bfloat16 [32, 256, 2048], P('fsdp')
- output 3: bfloat16 [32, 256, 2048], P('fsdp')
- output 4: float32 [32000, 2048], P('fsdp')
- output 5: float32 [2048], P('fsdp')
- output 6: float32 [2048, 2048], P('fsdp')
- output 7: float32 [2048, 2048], P('fsdp')
- output 8: float32 [2048, 2048], P('fsdp')
All inputs are finite; a program needn't handle non-finite values.
Results may differ from the reference program's by a relative error of at most 0.00413151.
Values are sent between devices in bfloat16 or wider.
A program may use at most 1 GiB of HBM per device.

```python
import math
import jax
import jax.numpy as jnp
from jax import lax

VOCAB_SIZE = 32000
MODEL_DIM = 2048
NUM_HEADS = 16
KV_HEADS = 16
HEAD_DIM = 128
BATCH_SIZE = 32
SEQ_LEN = 256


def draw_tokens(tok_key):
    num_levels = int(math.ceil(math.log2(VOCAB_SIZE)))
    level_key, id_key = jax.random.split(tok_key)
    tok_shape = (BATCH_SIZE, SEQ_LEN)
    tok_level = jax.random.randint(level_key, tok_shape, 0, num_levels + 1)
    id_upper = jnp.minimum(jnp.left_shift(jnp.ones(tok_shape, jnp.int32), tok_level), VOCAB_SIZE)
    token_ids = jax.random.randint(id_key, tok_shape, 0, id_upper)
    token_ids = token_ids.at[0, 0].set(0)
    return token_ids.at[BATCH_SIZE - 1, SEQ_LEN - 1].set(VOCAB_SIZE - 1)


def setup_inputs(seed: int = 0) -> dict:
    sub_keys = jax.random.split(jax.random.key(seed), 9)
    q_width = NUM_HEADS * HEAD_DIM
    kv_width = KV_HEADS * HEAD_DIM
    w_scale = MODEL_DIM ** -0.5
    cot_scale = (BATCH_SIZE * SEQ_LEN) ** -0.5
    act_shape = (BATCH_SIZE, SEQ_LEN)
    tokens = draw_tokens(sub_keys[0])
    embed_table = jax.random.normal(sub_keys[1], (VOCAB_SIZE, MODEL_DIM), jnp.float32)
    norm_gain = 1.0 + 0.3 * jax.random.normal(sub_keys[2], (MODEL_DIM,), jnp.float32)
    w_query = w_scale * jax.random.normal(sub_keys[3], (MODEL_DIM, q_width), jnp.float32)
    w_key = w_scale * jax.random.normal(sub_keys[4], (MODEL_DIM, kv_width), jnp.float32)
    w_value = w_scale * jax.random.normal(sub_keys[5], (MODEL_DIM, kv_width), jnp.float32)
    d_query = (cot_scale * jax.random.normal(sub_keys[6], act_shape + (q_width,), jnp.float32)).astype(jnp.bfloat16)
    d_key = (cot_scale * jax.random.normal(sub_keys[7], act_shape + (kv_width,), jnp.float32)).astype(jnp.bfloat16)
    d_value = (cot_scale * jax.random.normal(sub_keys[8], act_shape + (kv_width,), jnp.float32)).astype(jnp.bfloat16)
    return dict(tokens=tokens, embed_table=embed_table, norm_gain=norm_gain, w_query=w_query, w_key=w_key, w_value=w_value, d_query=d_query, d_key=d_key, d_value=d_value)


def reference(tokens, embed_table, norm_gain, w_query, w_key, w_value, d_query, d_key, d_value):
    w_query_bf = w_query.astype(jnp.bfloat16)
    w_key_bf = w_key.astype(jnp.bfloat16)
    w_value_bf = w_value.astype(jnp.bfloat16)

    def seq_step(acc_carry, row_in):
        grad_q, grad_k, grad_v, grad_gain = acc_carry
        tok_row, dq_row, dk_row, dv_row = row_in
        x_rows = embed_table[tok_row].astype(jnp.bfloat16).astype(jnp.float32)
        inv_rms = lax.rsqrt(jnp.mean(x_rows * x_rows, axis=-1, keepdims=True) + 1e-5)
        h_rows = x_rows * inv_rms
        normed = (h_rows * norm_gain).astype(jnp.bfloat16)
        q_rows = jnp.dot(normed, w_query_bf, preferred_element_type=jnp.float32).astype(jnp.bfloat16)
        k_rows = jnp.dot(normed, w_key_bf, preferred_element_type=jnp.float32).astype(jnp.bfloat16)
        v_rows = jnp.dot(normed, w_value_bf, preferred_element_type=jnp.float32).astype(jnp.bfloat16)
        grad_q = grad_q + jnp.dot(normed.T, dq_row, preferred_element_type=jnp.float32)
        grad_k = grad_k + jnp.dot(normed.T, dk_row, preferred_element_type=jnp.float32)
        grad_v = grad_v + jnp.dot(normed.T, dv_row, preferred_element_type=jnp.float32)
        d_normed = (jnp.dot(dq_row, w_query_bf.T, preferred_element_type=jnp.float32)
                    + jnp.dot(dk_row, w_key_bf.T, preferred_element_type=jnp.float32)
                    + jnp.dot(dv_row, w_value_bf.T, preferred_element_type=jnp.float32))
        grad_gain = grad_gain + jnp.sum(d_normed * h_rows, axis=0)
        u_rows = d_normed * norm_gain
        d_x = inv_rms * (u_rows - h_rows * jnp.mean(u_rows * h_rows, axis=-1, keepdims=True))
        return (grad_q, grad_k, grad_v, grad_gain), (q_rows, k_rows, v_rows, d_x)

    acc_init = (jnp.zeros(w_query.shape, jnp.float32), jnp.zeros(w_key.shape, jnp.float32),
                jnp.zeros(w_value.shape, jnp.float32), jnp.zeros(norm_gain.shape, jnp.float32))
    grad_sums, per_row = lax.scan(seq_step, acc_init, (tokens, d_query, d_key, d_value))
    query_proj, key_proj, value_proj, d_x_all = per_row
    d_embed = jnp.zeros(embed_table.shape, jnp.float32).at[tokens].add(d_x_all)
    grad_q, grad_k, grad_v, grad_gain = grad_sums
    return (query_proj, key_proj, value_proj, d_embed, grad_gain, grad_q, grad_k, grad_v)
```

```python
import functools, heapq
import jax
import jax.numpy as jnp
from jax import lax
from jax.experimental import pallas as pl
from jax.experimental.pallas import tpu as pltpu
from jax.sharding import PartitionSpec as P

AXIS_NAME = "fsdp"
NUM_DEV = 32
DIM_SIZE = {"z": 4, "y": 2, "x": 2}


def coords():
    me = lax.axis_index(AXIS_NAME)
    return me // 8, (me // 4) % 2, (me // 2) % 2, me % 2


def dev_at(z, y, x, c):
    return ((z * 2 + y) * 2 + x) * 2 + c


def neighbour(dim):
    z, y, x, c = coords()
    if dim == "z":
        return dev_at((z + 1) % 4, y, x, c)
    if dim == "y":
        return dev_at(z, 1 - y, x, c)
    if dim == "x":
        return dev_at(z, y, 1 - x, c)
    return dev_at(z, y, x, 1 - c)


def entry_barrier():
    me = lax.axis_index(AXIS_NAME)
    barrier = pltpu.get_barrier_semaphore()

    def signal(step, carry):
        pl.semaphore_signal(barrier, inc=1, device_id=((me + step) % NUM_DEV,), device_id_type=pl.DeviceIdType.MESH)
        return carry

    lax.fori_loop(1, NUM_DEV, signal, 0)
    pl.semaphore_wait(barrier, NUM_DEV - 1)


def remote(src, dst, send_sem, recv_sem, dev):
    return pltpu.make_async_remote_copy(src_ref=src, dst_ref=dst, send_sem=send_sem, recv_sem=recv_sem,
                                        device_id=(dev,), device_id_type=pl.DeviceIdType.MESH)


def hop_plan(parts, reduce):
    free = {"z": 0.0, "y": 0.0, "x": 0.0}
    hops = []
    for size, order in parts:
        seq, held = [], 1.0 if not reduce else 16.0
        for dim in order:
            n = DIM_SIZE[dim]
            if reduce:
                held /= n
            seq += [(dim, held * size)] * (n - 1)
            if not reduce:
                held *= n
        hops.append(seq)
    heap, events = [], []

    def issue(part, k, now):
        dim, cost = hops[part][k]
        free[dim] = max(free[dim], now) + cost
        heapq.heappush(heap, (free[dim], part, k))

    for part in range(len(parts)):
        issue(part, 0, 0.0)
    while heap:
        now, part, k = heapq.heappop(heap)
        events.append((part, k))
        if k + 1 < len(hops[part]):
            issue(part, k + 1, now)
    return events


def gather_steps(order):
    steps, whole = [], []
    for dim in order:
        for ring in range(DIM_SIZE[dim] - 1):
            steps.append((dim, ring, tuple(whole)))
        whole.append(dim)
    return steps


def box(dim, ring, whole, shift):
    z, y, x, _ = coords()
    pos = {"z": z, "y": y, "x": x}
    idx = []
    for d in ("z", "y", "x"):
        if d == dim:
            at = (pos[d] + 2 * DIM_SIZE[d] - ring - shift) % DIM_SIZE[d]
            idx.append(pl.ds(at, 1))
        elif d in whole:
            idx.append(pl.ds(0, DIM_SIZE[d]))
        else:
            idx.append(pl.ds(pos[d], 1))
    return tuple(idx)


def gather_kernel(parts, n_arr, *refs):
    ins, outs = refs[:n_arr], refs[n_arr:2 * n_arr]
    ssem, rsem, csem, dsem, lsem = refs[2 * n_arr:]
    z, y, x, c = coords()
    here = (pl.ds(z, 1), pl.ds(y, 1), pl.ds(x, 1))
    entry_barrier()
    partner = neighbour("c")

    def cut(arr, idx, core, part):
        _, col, ncol, _ = part
        return outs[arr].at[idx[0], idx[1], idx[2], pl.ds(core, 1), :, pl.ds(col, ncol)]

    def own(part):
        return ins[part[0]].at[:, :, :, :, :, pl.ds(part[1], part[2])]

    steps = [gather_steps(p[3]) for p in parts]

    def hop(i, k):
        dim, ring, whole = steps[i][k]
        idx = box(dim, ring, whole, 0)
        src = own(parts[i]) if k == 0 else cut(parts[i][0], idx, c, parts[i])
        return remote(src, cut(parts[i][0], idx, c, parts[i]), ssem.at[i, k], rsem.at[i, k], neighbour(dim))

    def cross(i, k):
        if k < 0:
            idx, src = here, own(parts[i])
        else:
            idx = box(*steps[i][k], 1)
            src = cut(parts[i][0], idx, c, parts[i])
        return remote(src, cut(parts[i][0], idx, c, parts[i]), csem.at[i, k + 1], dsem.at[i, k + 1], partner)

    local = [pltpu.make_async_copy(own(p), cut(p[0], here, c, p), lsem.at[i]) for i, p in enumerate(parts)]
    for i in range(len(parts)):
        hop(i, 0).start()
    for i in range(len(parts)):
        local[i].start()
        cross(i, -1).start()
    for i in range(len(parts)):
        local[i].wait()
    for i, k in hop_plan([(p[2] * p[4], p[3]) for p in [(*q, 1.0) for q in parts]], False):
        hop(i, k).wait_recv()
        if k + 1 < len(steps[i]):
            hop(i, k + 1).start()
        cross(i, k).start()
    for i in range(len(parts)):
        for k in range(-1, len(steps[i])):
            cross(i, k).wait()
        for k in range(len(steps[i])):
            hop(i, k).wait_send()


def all_gather_blocks(arrays, parts, collective_id):
    n = len(arrays)
    blocks = [a.reshape(1, 1, 1, 1, *a.shape) for a in arrays]
    np_ = len(parts)
    outs = pl.pallas_call(
        functools.partial(gather_kernel, parts, n),
        out_shape=[jax.ShapeDtypeStruct((4, 2, 2, 2, *a.shape), a.dtype) for a in arrays],
        in_specs=[pl.BlockSpec(memory_space=pltpu.VMEM)] * n,
        out_specs=[pl.BlockSpec(memory_space=pl.ANY)] * n,
        scratch_shapes=[pltpu.SemaphoreType.DMA((np_, 5)), pltpu.SemaphoreType.DMA((np_, 5)),
                        pltpu.SemaphoreType.DMA((np_, 6)), pltpu.SemaphoreType.DMA((np_, 6)),
                        pltpu.SemaphoreType.DMA((np_,))],
        compiler_params=pltpu.CompilerParams(collective_id=collective_id, has_side_effects=True),
        name="gather_blocks",
    )(*blocks)
    return [o.reshape(NUM_DEV * a.shape[0], a.shape[1]) for o, a in zip(outs, arrays)]


def add_into(dst, src, rows):
    lead = dst.shape[:-2]
    count = 1
    for n in lead:
        count *= n
    step = 8
    per = rows // step

    def body(t, carry):
        blk, off = t // per, pl.multiple_of((t % per) * step, step)
        idx = []
        for n in reversed(lead):
            idx.append(blk % n)
            blk = blk // n
        at = (*reversed(idx), pl.ds(off, step), slice(None))
        dst[at] = dst[at] + src[at]
        return carry

    lax.fori_loop(0, count * per, body, 0)


def scatter_steps(order):
    steps, done = [], []
    for dim in order:
        for ring in range(DIM_SIZE[dim] - 1):
            steps.append((dim, ring, tuple(done)))
        done.append(dim)
    return steps


def left_shape(done):
    return tuple(1 if d in done else DIM_SIZE[d] for d in ("z", "y", "x"))


def reduce_kernel(parts, n_arr, rows, collect, *refs):
    ins, outs = refs[:n_arr], refs[n_arr:2 * n_arr]
    rest = refs[2 * n_arr:]
    n_part = len(parts)
    recv = []
    at = 0
    for p in parts:
        recv.append(rest[at:at + 5])
        at += 5
    own_buf = []
    for p in parts:
        n_own = DIM_SIZE[p[3][0]] - 1
        own_buf.append(rest[at:at + n_own])
        at += n_own
    ssem, rsem, lsem, osem, tsem, usem = rest[at:at + 6]
    gsem = rest[at + 6] if collect else None
    z, y, x, c = coords()
    me = lax.axis_index(AXIS_NAME)
    pos = {"z": z, "y": y, "x": x}
    steps = [scatter_steps(p[3]) for p in parts]

    def pick(ref, dim, index):
        sel = [pl.ds(index, 1) if d == dim else slice(None) for d in ("z", "y", "x")]
        return ref.at[sel[0], sel[1], sel[2]]

    def first(i, dim, index):
        arr, col, ncol, _ = parts[i]
        sel = [pl.ds(index, 1) if d == dim else slice(None) for d in ("z", "y", "x")]
        return ins[arr].at[sel[0], sel[1], sel[2], :, pl.ds(col, ncol)]

    def held(i, dim, index, k):
        return first(i, dim, index) if k == 0 else pick(recv[i][k - 1], dim, index)

    def keep_index(dim, ring):
        n = DIM_SIZE[dim]
        return (pos[dim] + 2 * n - ring - 2) % n if n > 2 else pos[dim]

    def hop(i, k):
        dim, ring, _ = steps[i][k]
        n = DIM_SIZE[dim]
        if ring == 0:
            src = held(i, dim, (pos[dim] + n - 1) % n, k)
        else:
            src = recv[i][k - 1]
        return remote(src, recv[i][k], ssem.at[i, k], rsem.at[i, k], neighbour(dim))

    def load(i, k):
        dim, ring, _ = steps[i][k]
        return pltpu.make_async_copy(first(i, dim, keep_index(dim, ring)), own_buf[i][k], lsem.at[i, k])

    entry_barrier()
    for i in range(n_part):
        hop(i, 0).start()
    for i in range(n_part):
        for k in range(len(own_buf[i])):
            load(i, k).start()

    def finish(i):
        arr, col, ncol, _ = parts[i]
        acc = recv[i][4]
        r = rows[arr]
        if arr in collect:
            idx = (pl.ds(z, 1), pl.ds(y, 1), pl.ds(x, 1), slice(None), pl.ds(c * collect[arr] + col, ncol))
            dst = outs[arr].at[idx]

            @pl.when(me != 0)
            def _():
                remote(acc, dst, tsem.at[i], gsem.at[i, me], 0).start()

            @pl.when(me == 0)
            def _():
                pltpu.make_async_copy(acc, dst, osem.at[i]).start()
            return
        half = r // 2
        cols = pl.ds(c * (outs[arr].shape[-1] // 2) + col, ncol)
        dst = outs[arr].at[:, :, :, :, cols]
        mine = acc.at[:, :, :, pl.ds(c * half, half), :]
        theirs = acc.at[:, :, :, pl.ds((1 - c) * half, half), :]
        remote(theirs, dst, tsem.at[i], usem.at[i], neighbour("c")).start()
        pltpu.make_async_copy(mine, dst, osem.at[i]).start()

    def finish_wait(i):
        arr, col, ncol, _ = parts[i]
        acc = recv[i][4]
        r = rows[arr]
        if arr in collect:
            dst = outs[arr].at[pl.ds(z, 1), pl.ds(y, 1), pl.ds(x, 1), :, pl.ds(c * collect[arr] + col, ncol)]

            @pl.when(me != 0)
            def _():
                remote(acc, dst, tsem.at[i], gsem.at[i, me], 0).wait_send()

            @pl.when(me == 0)
            def _():
                pltpu.make_async_copy(acc, dst, osem.at[i]).wait()

                def one(s, carry):
                    from_at = outs[arr].at[pl.ds(s // 8, 1), pl.ds((s // 4) % 2, 1), pl.ds((s // 2) % 2, 1), :,
                                           pl.ds(pl.multiple_of((s % 2) * collect[arr] + col, 128), ncol)]
                    remote(acc, from_at, tsem.at[i], gsem.at[i, s], 0).wait_recv()
                    return carry

                lax.fori_loop(1, NUM_DEV, one, 0)
            return
        half = r // 2
        cols = pl.ds(c * (outs[arr].shape[-1] // 2) + col, ncol)
        dst = outs[arr].at[:, :, :, :, cols]
        mine = acc.at[:, :, :, pl.ds(c * half, half), :]
        theirs = acc.at[:, :, :, pl.ds((1 - c) * half, half), :]
        remote(theirs, dst, tsem.at[i], usem.at[i], neighbour("c")).wait()
        pltpu.make_async_copy(mine, dst, osem.at[i]).wait()

    cost = [p[2] * rows[p[0]] for p in parts]
    for i, k in hop_plan(list(zip(cost, [p[3] for p in parts])), True):
        dim, ring, _ = steps[i][k]
        start = k - ring
        hop(i, k).wait_recv()
        if k < len(own_buf[i]):
            load(i, k).wait()
            src = own_buf[i][k]
        else:
            src = held(i, dim, keep_index(dim, ring), start)
        add_into(recv[i][k], src, rows[parts[i][0]])
        if k + 1 < 5:
            hop(i, k + 1).start()
        else:
            finish(i)
    for i in range(n_part):
        for k in range(5):
            hop(i, k).wait_send()
        finish_wait(i)


def reduce_scatter_blocks(arrays, parts, collect, collective_id):
    n = len(arrays)
    rows = [a.shape[0] // 16 for a in arrays]
    ins = [a.reshape(4, 2, 2, r, a.shape[1]) for a, r in zip(arrays, rows)]
    scratch = []
    for p in parts:
        for dim, ring, done in scatter_steps(p[3]):
            scratch.append(pltpu.VMEM((*left_shape(done + (dim,)), rows[p[0]], p[2]), jnp.float32))
    for p in parts:
        for k in range(DIM_SIZE[p[3][0]] - 1):
            scratch.append(pltpu.VMEM((*left_shape((p[3][0],)), rows[p[0]], p[2]), jnp.float32))
    m = len(parts)
    scratch += [pltpu.SemaphoreType.DMA((m, 5)), pltpu.SemaphoreType.DMA((m, 5)), pltpu.SemaphoreType.DMA((m, 3)),
                pltpu.SemaphoreType.DMA((m,)), pltpu.SemaphoreType.DMA((m,)), pltpu.SemaphoreType.DMA((m,))]
    out_shape = []
    for i, a in enumerate(arrays):
        if i in collect:
            out_shape.append(jax.ShapeDtypeStruct((4, 2, 2, rows[i], 2 * a.shape[1]), jnp.float32))
        else:
            out_shape.append(jax.ShapeDtypeStruct((1, 1, 1, rows[i] // 2, 2 * a.shape[1]), jnp.float32))
    if collect:
        scratch.append(pltpu.SemaphoreType.DMA((m, NUM_DEV)))
    outs = pl.pallas_call(
        functools.partial(reduce_kernel, parts, n, rows, {i: arrays[i].shape[1] for i in collect}),
        out_shape=out_shape,
        in_specs=[pl.BlockSpec(memory_space=pl.ANY)] * n,
        out_specs=[pl.BlockSpec(memory_space=pl.ANY)] * n,
        scratch_shapes=scratch,
        compiler_params=pltpu.CompilerParams(collective_id=collective_id, has_side_effects=True, vmem_limit_bytes=60 * 2**20),
        name="reduce_blocks",
    )(*ins)
    return [o.reshape(-1, o.shape[-1]) for o in outs]


def exchange_kernel(n_arr, has_hot, *refs):
    n_in = n_arr + has_hot
    srcs, dsts = refs[:n_arr], refs[n_in:n_in + n_arr]
    ssem, rsem, lsem = refs[2 * n_in:2 * n_in + 3]
    if has_hot:
        hot, hot_dst = refs[n_arr], refs[n_in + n_arr]
        hsem, gsem = refs[2 * n_in + 3:]
    me = lax.axis_index(AXIS_NAME)
    entry_barrier()

    def copy(a, step):
        to = (me + step) % NUM_DEV
        return remote(srcs[a].at[pl.ds(to, 1)], dsts[a].at[pl.ds(me, 1)], ssem.at[a, step], rsem.at[a, step], to)

    def local(a):
        return pltpu.make_async_copy(srcs[a].at[pl.ds(me, 1)], dsts[a].at[pl.ds(me, 1)], lsem.at[a])

    def hot_copy(to):
        return remote(hot.at[pl.ds(to, 1)], hot_dst, hsem.at[to], gsem, to)

    def start(step, carry):
        for a in range(n_arr):
            copy(a, step).start()
        return carry

    lax.fori_loop(1, NUM_DEV, start, 0)
    for a in range(n_arr):
        local(a).start()
    if has_hot:
        @pl.when(me == 0)
        def _():
            def hot_start(to, carry):
                hot_copy(to).start()
                return carry

            lax.fori_loop(1, NUM_DEV, hot_start, 0)
            mine = pltpu.make_async_copy(hot.at[pl.ds(0, 1)], hot_dst, lsem.at[n_arr])
            mine.start()
            mine.wait()

    def finish(step, carry):
        for a in range(n_arr):
            copy(a, step).wait()
        return carry

    lax.fori_loop(1, NUM_DEV, finish, 0)
    for a in range(n_arr):
        local(a).wait()
    if has_hot:
        @pl.when(me == 0)
        def _():
            def hot_end(to, carry):
                hot_copy(to).wait_send()
                return carry

            lax.fori_loop(1, NUM_DEV, hot_end, 0)

        @pl.when(me != 0)
        def _():
            hot_copy(0).wait_recv()


def exchange(blocks, hot, collective_id):
    any_spec = pl.BlockSpec(memory_space=pl.ANY)
    n = len(blocks)
    sems = [pltpu.SemaphoreType.DMA((n, NUM_DEV)), pltpu.SemaphoreType.DMA((n, NUM_DEV)), pltpu.SemaphoreType.DMA((n + 1,))]
    out_shape = [jax.ShapeDtypeStruct(b.shape, b.dtype) for b in blocks]
    args = list(blocks)
    if hot is not None:
        out_shape.append(jax.ShapeDtypeStruct((1, *hot.shape[1:]), hot.dtype))
        sems += [pltpu.SemaphoreType.DMA((NUM_DEV,)), pltpu.SemaphoreType.DMA]
        args.append(hot)
    return pl.pallas_call(
        functools.partial(exchange_kernel, n, int(hot is not None)),
        out_shape=out_shape,
        in_specs=[any_spec] * len(args),
        out_specs=[any_spec] * len(args),
        scratch_shapes=sems,
        compiler_params=pltpu.CompilerParams(collective_id=collective_id, has_side_effects=True),
        name="exchange",
    )(*args)


BLOCK = 8
MOST = 4
WIDE_OWNERS = ((1, 4, 4), (4, 9, 2))


def owner_blocks(owner):
    blocks = jnp.ones_like(owner)
    for first, last, n in WIDE_OWNERS:
        blocks = jnp.where((owner >= first) & (owner < last), n, blocks)
    return blocks


def cold_kernel(to_owner, src, dst, ssem, rsem):
    me = lax.axis_index(AXIS_NAME)
    entry_barrier()

    def copy(step, n):
        to = (me + step) % NUM_DEV
        return remote(src.at[pl.ds(to, 1), pl.ds(0, n)], dst.at[pl.ds(me, 1), pl.ds(0, n)], ssem.at[step], rsem.at[step], to)

    def by_size(owner, do):
        wide = owner < 0
        for first, last, n in WIDE_OWNERS:
            hit = (owner >= first) & (owner < last)
            wide = wide | hit
            pl.when(hit)(functools.partial(do, n))
        pl.when(jnp.logical_not(wide))(functools.partial(do, 1))

    def start(step, carry):
        by_size((me + step) % NUM_DEV if to_owner else me, lambda n: copy(step, n).start())
        return carry

    def finish(step, carry):
        by_size((me + step) % NUM_DEV if to_owner else me, lambda n: copy(step, n).wait_send())
        by_size(me if to_owner else (me - step + NUM_DEV) % NUM_DEV, lambda n: copy(step, n).wait_recv())
        return carry

    lax.fori_loop(1, NUM_DEV, start, 0)
    lax.fori_loop(1, NUM_DEV, finish, 0)


def cold_exchange(blocks, to_owner, collective_id):
    any_spec = pl.BlockSpec(memory_space=pl.ANY)
    return pl.pallas_call(
        functools.partial(cold_kernel, to_owner),
        out_shape=jax.ShapeDtypeStruct(blocks.shape, blocks.dtype),
        in_specs=[any_spec], out_specs=any_spec,
        scratch_shapes=[pltpu.SemaphoreType.DMA((NUM_DEV,)), pltpu.SemaphoreType.DMA((NUM_DEV,))],
        compiler_params=pltpu.CompilerParams(collective_id=collective_id, has_side_effects=True),
        name="cold_to_owner" if to_owner else "cold_to_device",
    )(blocks)


CAP = BLOCK * MOST


def add_kernel(ids, first, count, base, acc, rows, out, buf, sem, asem):
    def get(d, g):
        return pltpu.make_async_copy(rows.at[d, g], buf.at[d, g], sem.at[d, g])

    def each(do):
        def device(d, carry):
            def group(g, inner):
                do(d, g)
                return inner

            return lax.fori_loop(0, (count[d] + BLOCK - 1) // BLOCK, group, carry)

        lax.fori_loop(0, NUM_DEV, device, 0)

    each(lambda d, g: get(d, g).start())
    copy = pltpu.make_async_copy(acc, out, asem.at[0])
    copy.start()
    copy.wait()

    def add(d, g):
        get(d, g).wait()

        def row(r, carry):
            at = jnp.clip(ids[d, first[d] + BLOCK * g + r] - base[0], 0, out.shape[0] - 1)
            out[pl.ds(at, 1), :] += buf[d, g, pl.ds(r, 1), :]
            return carry

        lax.fori_loop(0, jnp.minimum(count[d] - BLOCK * g, BLOCK), row, 0)

    each(add)


def add_rows(ids, first, count, base, acc, rows):
    any_spec = pl.BlockSpec(memory_space=pl.ANY)
    return pl.pallas_call(
        add_kernel,
        out_shape=jax.ShapeDtypeStruct(acc.shape, jnp.float32),
        grid_spec=pltpu.PrefetchScalarGridSpec(
            num_scalar_prefetch=4, grid=(1,),
            in_specs=[any_spec, any_spec],
            out_specs=pl.BlockSpec(acc.shape, lambda i, *_: (0, 0)),
            scratch_shapes=[pltpu.VMEM((NUM_DEV, MOST, BLOCK, acc.shape[1]), jnp.float32),
                            pltpu.SemaphoreType.DMA((NUM_DEV, MOST)), pltpu.SemaphoreType.DMA((1,))]),
        compiler_params=pltpu.CompilerParams(vmem_limit_bytes=40 * 2**20),
        name="add_rows",
    )(ids, first, count, base, acc, rows)


GATHER_PARTS = [(0, 0, 1024, "xyz"), (0, 1024, 1024, "zyx"), (1, 0, 1024, "zxy"), (1, 1024, 1024, "zyx"),
                (2, 0, 1024, "zxy"), (2, 1024, 1024, "yxz"), (3, 0, 2048, "zxy")]
REDUCE_PARTS = [(3, 0, 1024, "xyz"), (0, 0, 1024, "yxz"), (1, 0, 1024, "xyz"), (2, 0, 512, "zxy"), (2, 512, 512, "yxz")]
HOT_ROWS = 1024


def norm_forward(x_rows, gain_full):
    inv_rms = lax.rsqrt(jnp.mean(x_rows * x_rows, axis=-1, keepdims=True) + 1e-5)
    h_rows = x_rows * inv_rms
    return inv_rms, h_rows, (h_rows * gain_full).astype(jnp.bfloat16)


def dot(a, b, dims, precision=None):
    return lax.dot_general(a, b, (dims, ((), ())), preferred_element_type=jnp.float32, precision=precision)


def solution(mesh):
    def local_step(tokens, embed_shard, gain_shard, wq_shard, wk_shard, wv_shard, d_query, d_key, d_value):
        vocab_local, width = embed_shard.shape
        n_tok = tokens.shape[1]
        me = lax.axis_index(AXIS_NAME)
        core = me % 2
        swap = [(d, d ^ 1) for d in range(NUM_DEV)]
        half = width // 2

        def partner(a):
            return lax.ppermute(a, AXIS_NAME, swap)

        def my_half(a, c):
            return lax.dynamic_slice_in_dim(a, c * half, half, axis=1)

        def paired(a):
            return jnp.concatenate([my_half(a, core), partner(my_half(a, 1 - core))], axis=0)

        tok = tokens[0]
        pos = jnp.arange(n_tok, dtype=jnp.int32)
        before = (tok[None, :] < tok[:, None]) | ((tok[None, :] == tok[:, None]) & (pos[None, :] < pos[:, None]))
        rank = jnp.sum(before.astype(jnp.int32), axis=1)
        place = rank[None, :] == pos[:, None]
        sorted_ids = jnp.sum(jnp.where(place, tok[None, :], 0), axis=1)

        hot_own = jnp.pad(embed_shard.astype(jnp.bfloat16), ((0, HOT_ROWS - vocab_local), (0, 0)))
        gain_rows = gain_shard.shape[0]
        ids_all, gains, hot_block = exchange(
            [jnp.broadcast_to(sorted_ids.reshape(1, 2, 128), (NUM_DEV, 2, 128)),
             jnp.broadcast_to(jnp.pad(gain_shard, (0, 128 - gain_rows)), (NUM_DEV, 1, 128))],
            hot_own.reshape(NUM_DEV, HOT_ROWS // NUM_DEV, width), 4)
        gain_full = gains[:, 0, :gain_rows].reshape(-1)
        ids_all = ids_all.reshape(NUM_DEV, n_tok)
        limits = vocab_local * jnp.arange(NUM_DEV + 1, dtype=jnp.int32)
        starts = jnp.sum((ids_all[:, :, None] < limits).astype(jnp.int32), axis=1)
        counts = (starts[:, 1:] - starts[:, :-1]).at[:, 0].set(0)
        owner_first = lax.dynamic_index_in_dim(starts, me, axis=1, keepdims=False)
        owner_count = lax.dynamic_index_in_dim(counts, me, axis=1, keepdims=False)
        my_first = lax.dynamic_index_in_dim(starts, me, axis=0, keepdims=False)[:NUM_DEV]
        my_count = lax.dynamic_index_in_dim(counts, me, axis=0, keepdims=False)
        base = (me * vocab_local).reshape(1)
        owners = jnp.arange(NUM_DEV, dtype=jnp.int32)
        slot = jnp.arange(CAP, dtype=jnp.int32)
        caps = BLOCK * owner_blocks(owners)
        my_cap = BLOCK * owner_blocks(me)
        rounds = jnp.maximum(jnp.max((counts + caps - 1) // caps), 1)
        tok_owner = tok // vocab_local
        tok_slot = rank - jnp.sum(jnp.where(tok_owner[:, None] == owners, my_first, 0), axis=1)
        tok_cap = BLOCK * owner_blocks(tok_owner)

        def cold_round(carry):
            step, cold = carry
            want = owner_first[:, None] + step * my_cap + slot
            ids = jnp.sum(jnp.where(want[:, :, None] == pos, ids_all[:, None, :], 0), axis=2) - base
            rows = jnp.take(embed_shard, jnp.clip(ids, 0, vocab_local - 1).reshape(-1), axis=0).astype(jnp.bfloat16)
            got = cold_exchange(rows.reshape(NUM_DEV, MOST, BLOCK, width), False, 6).reshape(-1, width)
            at = tok_slot - step * tok_cap
            here = (tok_owner > 0) & (at >= 0) & (at < tok_cap)
            mine = jnp.take(got, jnp.where(here, tok_owner * CAP + at, 0), axis=0)
            own = (tok_owner == me)[:, None]
            mine = jnp.where(own, jnp.take(rows, jnp.where(here, me * CAP + at, 0), axis=0), mine)
            return step + 1, jnp.where(here[:, None], mine, cold)

        _, cold = lax.while_loop(lambda carry: carry[0] < rounds, cold_round,
                                 (jnp.int32(0), jnp.zeros((n_tok, width), jnp.bfloat16)))

        shards = [w.astype(jnp.bfloat16) for w in (wq_shard, wk_shard, wv_shard)]
        wq_full, wk_full, wv_full, hot = all_gather_blocks([*shards, hot_block[0]], GATHER_PARTS, 1)

        hot_sel = ((tok[:, None] == jnp.arange(HOT_ROWS, dtype=jnp.int32)) & (tok[:, None] < vocab_local)).astype(jnp.bfloat16)
        x_rows = dot(hot_sel, hot, ((1,), (0,))) + cold.astype(jnp.float32)
        inv_rms, h_rows, normed = norm_forward(x_rows, gain_full)
        dq, dk, dv = d_query[0], d_key[0], d_value[0]
        normed_pair = jnp.concatenate([normed, partner(normed)], axis=0)
        d_w = [dot(normed_pair, paired(d), ((0,), (0,))) for d in (dq, dk, dv)]
        query_proj, key_proj, value_proj = [dot(normed, w, ((1,), (0,))).astype(jnp.bfloat16)[None]
                                            for w in (wq_full, wk_full, wv_full)]
        d_normed = (dot(dq, wq_full, ((1,), (1,))) + dot(dk, wk_full, ((1,), (1,))) + dot(dv, wv_full, ((1,), (1,))))
        gain_part = jnp.sum(d_normed * h_rows, axis=0)
        u_rows = d_normed * gain_full
        d_x = inv_rms * (u_rows - h_rows * jnp.mean(u_rows * h_rows, axis=-1, keepdims=True))

        pair_ids = jnp.concatenate([tok, partner(tok)])
        pair_sel = ((pair_ids[:, None] == jnp.arange(HOT_ROWS, dtype=jnp.int32)) & (pair_ids[:, None] < vocab_local)).astype(jnp.float32)
        hot_part = dot(pair_sel, paired(d_x), ((0,), (0,)), lax.Precision.HIGHEST)
        d_w_query, d_w_key, d_w_value, hot_sum = reduce_scatter_blocks([*d_w, hot_part], REDUCE_PARTS, (3,), 2)

        gain_blocks = jnp.pad(gain_part.reshape(NUM_DEV, 1, -1), ((0, 0), (0, 0), (0, 128 - gain_rows)))
        d_norm_gain = jnp.sum(exchange([gain_blocks], None, 5)[0], axis=(0, 1))[:gain_rows]
        d_embed = jnp.where(me == 0, hot_sum[:vocab_local], 0.0)

        def add_round(carry):
            step, total = carry
            want = my_first[:, None] + step * caps[:, None] + slot
            src = jnp.sum(jnp.where(want[:, :, None] == rank, pos, 0), axis=2)
            rows = jnp.take(d_x, src.reshape(-1), axis=0).reshape(NUM_DEV, MOST, BLOCK, width)
            got = cold_exchange(rows, True, 7)
            got = lax.dynamic_update_slice_in_dim(got, lax.dynamic_slice_in_dim(rows, me, 1, axis=0), me, axis=0)
            left = jnp.clip(owner_count - step * my_cap, 0, my_cap)
            return step + 1, add_rows(ids_all, owner_first + step * my_cap, left, base, total, got)

        _, d_embed = lax.while_loop(lambda carry: carry[0] < rounds, add_round, (jnp.int32(0), d_embed))
        return (query_proj, key_proj, value_proj, d_embed, d_norm_gain, d_w_query, d_w_key, d_w_value)

    row_spec = P(AXIS_NAME, None)
    act_spec = P(AXIS_NAME, None, None)
    vec_spec = P(AXIS_NAME)
    return jax.shard_map(local_step, mesh=mesh,
                         in_specs=(row_spec, row_spec, vec_spec, row_spec, row_spec, row_spec, act_spec, act_spec, act_spec),
                         out_specs=(act_spec, act_spec, act_spec, row_spec, vec_spec, row_spec, row_spec, row_spec),
                         check_vma=False)
```

```python
import functools
import jax
import jax.numpy as jnp
from jax import lax
from jax.experimental import pallas as pl
from jax.experimental.pallas import tpu as pltpu
from jax.sharding import PartitionSpec as P

AXIS_NAME = "fsdp"
NUM_DEV = 32
DIM_SIZE = {"z": 4, "y": 2, "x": 2}


def coords():
    me = lax.axis_index(AXIS_NAME)
    return me // 8, (me // 4) % 2, (me // 2) % 2, me % 2


def dev_at(z, y, x, c):
    return ((z * 2 + y) * 2 + x) * 2 + c


def neighbour(dim):
    z, y, x, c = coords()
    if dim == "z":
        return dev_at((z + 1) % 4, y, x, c)
    if dim == "y":
        return dev_at(z, 1 - y, x, c)
    if dim == "x":
        return dev_at(z, y, 1 - x, c)
    return dev_at(z, y, x, 1 - c)


def entry_barrier():
    me = lax.axis_index(AXIS_NAME)
    barrier = pltpu.get_barrier_semaphore()

    def signal(step, carry):
        pl.semaphore_signal(barrier, inc=1, device_id=((me + step) % NUM_DEV,), device_id_type=pl.DeviceIdType.MESH)
        return carry

    lax.fori_loop(1, NUM_DEV, signal, 0)
    pl.semaphore_wait(barrier, NUM_DEV - 1)


def remote(src, dst, send_sem, recv_sem, dev):
    return pltpu.make_async_remote_copy(src_ref=src, dst_ref=dst, send_sem=send_sem, recv_sem=recv_sem,
                                        device_id=(dev,), device_id_type=pl.DeviceIdType.MESH)


def gather_steps(order):
    steps, whole = [], []
    for dim in order:
        for ring in range(DIM_SIZE[dim] - 1):
            steps.append((dim, ring, tuple(whole)))
        whole.append(dim)
    return steps


def box(dim, ring, whole, shift):
    z, y, x, _ = coords()
    pos = {"z": z, "y": y, "x": x}
    idx = []
    for d in ("z", "y", "x"):
        if d == dim:
            at = (pos[d] + 2 * DIM_SIZE[d] - ring - shift) % DIM_SIZE[d]
            idx.append(pl.ds(at, 1))
        elif d in whole:
            idx.append(pl.ds(0, DIM_SIZE[d]))
        else:
            idx.append(pl.ds(pos[d], 1))
    return tuple(idx)


def gather_kernel(parts, first, events, n_arr, *refs):
    ins, outs = refs[:n_arr], refs[n_arr:2 * n_arr]
    ssem, rsem, csem, dsem, lsem = refs[2 * n_arr:]
    z, y, x, c = coords()
    me = lax.axis_index(AXIS_NAME)
    here = (pl.ds(z, 1), pl.ds(y, 1), pl.ds(x, 1))
    entry_barrier()
    partner = neighbour("c")

    def cut(arr, idx, core, part):
        _, col, ncol, _ = part
        return outs[arr].at[idx[0], idx[1], idx[2], pl.ds(core, 1), :, pl.ds(col, ncol)]

    def own(part):
        return ins[part[0]].at[:, :, :, :, :, pl.ds(part[1], part[2])]

    steps = [gather_steps(p[3]) for p in parts]

    def hop(i, k):
        dim, ring, whole = steps[i][k]
        idx = box(dim, ring, whole, 0)
        src = own(parts[i]) if k == 0 else cut(parts[i][0], idx, c, parts[i])
        return remote(src, cut(parts[i][0], idx, c, parts[i]), ssem.at[i, k], rsem.at[i, k], neighbour(dim))

    def cross(i, k):
        if k < 0:
            idx, src = here, own(parts[i])
        else:
            idx = box(*steps[i][k], 1)
            src = cut(parts[i][0], idx, c, parts[i])
        return remote(src, cut(parts[i][0], idx, c, parts[i]), csem.at[i, k + 1], dsem.at[i, k + 1], partner)

    def local(i):
        return pltpu.make_async_copy(own(parts[i]), cut(parts[i][0], here, c, parts[i]), lsem.at[i])

    for i in first:
        hop(i, 0).start()
    for i in first:
        local(i).start()
        cross(i, -1).start()
    for i in first:
        local(i).wait()
    for i, k in events:
        if k < 0:
            hop(i, 0).start()
            local(i).start()
            cross(i, -1).start()
            local(i).wait()
            continue
        hop(i, k).wait_recv()
        if k + 1 < len(steps[i]):
            hop(i, k + 1).start()
        cross(i, k).start()
    for i in range(len(parts)):
        for k in range(-1, len(steps[i])):
            cross(i, k).wait()
        for k in range(len(steps[i])):
            hop(i, k).wait_send()


def all_gather_blocks(blocks, plan, collective_id):
    parts, first, events = plan
    n, m = len(blocks), len(parts)
    outs = pl.pallas_call(
        functools.partial(gather_kernel, parts, first, events, n),
        out_shape=[jax.ShapeDtypeStruct((4, 2, 2, 2, *b.shape), b.dtype) for b in blocks],
        in_specs=[pl.BlockSpec(memory_space=pltpu.VMEM)] * n,
        out_specs=[pl.BlockSpec(memory_space=pl.ANY)] * n,
        scratch_shapes=[pltpu.SemaphoreType.DMA((m, 5)), pltpu.SemaphoreType.DMA((m, 5)),
                        pltpu.SemaphoreType.DMA((m, 6)), pltpu.SemaphoreType.DMA((m, 6)), pltpu.SemaphoreType.DMA((m,))],
        compiler_params=pltpu.CompilerParams(collective_id=collective_id, has_side_effects=True),
        name="gather_blocks",
    )(*[b.reshape(1, 1, 1, 1, *b.shape) for b in blocks])
    return [o.reshape(NUM_DEV * b.shape[0], b.shape[1]) for o, b in zip(outs, blocks)]


def add_into(dst, src, rows):
    lead = dst.shape[:-2]
    count = 1
    for n in lead:
        count *= n
    step = 8
    per = rows // step

    def body(t, carry):
        blk, off = t // per, pl.multiple_of((t % per) * step, step)
        idx = []
        for n in reversed(lead):
            idx.append(blk % n)
            blk = blk // n
        at = (*reversed(idx), pl.ds(off, step), slice(None))
        dst[at] = dst[at] + src[at]
        return carry

    lax.fori_loop(0, count * per, body, 0)


def scatter_steps(order):
    steps, done = [], []
    for dim in order:
        for ring in range(DIM_SIZE[dim] - 1):
            steps.append((dim, ring, tuple(done)))
        done.append(dim)
    return steps


def left_shape(done):
    return tuple(1 if d in done else DIM_SIZE[d] for d in ("z", "y", "x"))


def reduce_kernel(parts, first_hops, events, n_arr, rows, collect, *refs):
    ins, outs = refs[:n_arr], refs[n_arr:2 * n_arr]
    rest = refs[2 * n_arr:]
    n_part = len(parts)
    recv = []
    at = 0
    for p in parts:
        recv.append(rest[at:at + 5])
        at += 5
    own_buf = []
    for p in parts:
        n_own = DIM_SIZE[p[3][0]] - 1
        own_buf.append(rest[at:at + n_own])
        at += n_own
    ssem, rsem, lsem, osem, tsem, usem = rest[at:at + 6]
    gsem = rest[at + 6] if collect else None
    z, y, x, c = coords()
    me = lax.axis_index(AXIS_NAME)
    pos = {"z": z, "y": y, "x": x}
    steps = [scatter_steps(p[3]) for p in parts]

    def pick(ref, dim, index):
        sel = [pl.ds(index, 1) if d == dim else slice(None) for d in ("z", "y", "x")]
        return ref.at[sel[0], sel[1], sel[2]]

    def first(i, dim, index):
        arr, col, ncol, _ = parts[i]
        sel = [pl.ds(index, 1) if d == dim else slice(None) for d in ("z", "y", "x")]
        return ins[arr].at[sel[0], sel[1], sel[2], :, pl.ds(col, ncol)]

    def held(i, dim, index, k):
        return first(i, dim, index) if k == 0 else pick(recv[i][k - 1], dim, index)

    def keep_index(dim, ring):
        n = DIM_SIZE[dim]
        return (pos[dim] + 2 * n - ring - 2) % n if n > 2 else pos[dim]

    def hop(i, k):
        dim, ring, _ = steps[i][k]
        n = DIM_SIZE[dim]
        if ring == 0:
            src = held(i, dim, (pos[dim] + n - 1) % n, k)
        else:
            src = recv[i][k - 1]
        return remote(src, recv[i][k], ssem.at[i, k], rsem.at[i, k], neighbour(dim))

    def load(i, k):
        dim, ring, _ = steps[i][k]
        return pltpu.make_async_copy(first(i, dim, keep_index(dim, ring)), own_buf[i][k], lsem.at[i, k])

    entry_barrier()
    for i in first_hops:
        hop(i, 0).start()
    for i in first_hops:
        for k in range(len(own_buf[i])):
            load(i, k).start()

    def finish(i):
        arr, col, ncol, _ = parts[i]
        acc = recv[i][4]
        r = rows[arr]
        if arr in collect:
            idx = (pl.ds(z, 1), pl.ds(y, 1), pl.ds(x, 1), slice(None), pl.ds(c * collect[arr] + col, ncol))
            dst = outs[arr].at[idx]

            @pl.when(me != 0)
            def _():
                remote(acc, dst, tsem.at[i], gsem.at[i, me], 0).start()

            @pl.when(me == 0)
            def _():
                pltpu.make_async_copy(acc, dst, osem.at[i]).start()
            return
        half = r // 2
        cols = pl.ds(c * (outs[arr].shape[-1] // 2) + col, ncol)
        dst = outs[arr].at[:, :, :, :, cols]
        mine = acc.at[:, :, :, pl.ds(c * half, half), :]
        theirs = acc.at[:, :, :, pl.ds((1 - c) * half, half), :]
        remote(theirs, dst, tsem.at[i], usem.at[i], neighbour("c")).start()
        pltpu.make_async_copy(mine, dst, osem.at[i]).start()

    def finish_wait(i):
        arr, col, ncol, _ = parts[i]
        acc = recv[i][4]
        r = rows[arr]
        if arr in collect:
            dst = outs[arr].at[pl.ds(z, 1), pl.ds(y, 1), pl.ds(x, 1), :, pl.ds(c * collect[arr] + col, ncol)]

            @pl.when(me != 0)
            def _():
                remote(acc, dst, tsem.at[i], gsem.at[i, me], 0).wait_send()

            @pl.when(me == 0)
            def _():
                pltpu.make_async_copy(acc, dst, osem.at[i]).wait()

                def one(s, carry):
                    from_at = outs[arr].at[pl.ds(s // 8, 1), pl.ds((s // 4) % 2, 1), pl.ds((s // 2) % 2, 1), :,
                                           pl.ds(pl.multiple_of((s % 2) * collect[arr] + col, 128), ncol)]
                    remote(acc, from_at, tsem.at[i], gsem.at[i, s], 0).wait_recv()
                    return carry

                lax.fori_loop(1, NUM_DEV, one, 0)
            return
        half = r // 2
        cols = pl.ds(c * (outs[arr].shape[-1] // 2) + col, ncol)
        dst = outs[arr].at[:, :, :, :, cols]
        mine = acc.at[:, :, :, pl.ds(c * half, half), :]
        theirs = acc.at[:, :, :, pl.ds((1 - c) * half, half), :]
        remote(theirs, dst, tsem.at[i], usem.at[i], neighbour("c")).wait()
        pltpu.make_async_copy(mine, dst, osem.at[i]).wait()

    for i, k in events:
        dim, ring, _ = steps[i][k]
        start = k - ring
        hop(i, k).wait_recv()
        if k < len(own_buf[i]):
            load(i, k).wait()
            src = own_buf[i][k]
        else:
            src = held(i, dim, keep_index(dim, ring), start)
        add_into(recv[i][k], src, rows[parts[i][0]])
        if k + 1 < 5:
            hop(i, k + 1).start()
        else:
            finish(i)
    for i in range(n_part):
        for k in range(5):
            hop(i, k).wait_send()
        finish_wait(i)


def reduce_scatter_blocks(arrays, plan, collect, collective_id):
    parts, first, events = plan
    n = len(arrays)
    rows = [a.shape[0] // 16 for a in arrays]
    ins = [a.reshape(4, 2, 2, r, a.shape[1]) for a, r in zip(arrays, rows)]
    scratch = []
    for p in parts:
        for dim, ring, done in scatter_steps(p[3]):
            scratch.append(pltpu.VMEM((*left_shape(done + (dim,)), rows[p[0]], p[2]), jnp.float32))
    for p in parts:
        for k in range(DIM_SIZE[p[3][0]] - 1):
            scratch.append(pltpu.VMEM((*left_shape((p[3][0],)), rows[p[0]], p[2]), jnp.float32))
    m = len(parts)
    scratch += [pltpu.SemaphoreType.DMA((m, 5)), pltpu.SemaphoreType.DMA((m, 5)), pltpu.SemaphoreType.DMA((m, 3)),
                pltpu.SemaphoreType.DMA((m,)), pltpu.SemaphoreType.DMA((m,)), pltpu.SemaphoreType.DMA((m,))]
    out_shape = []
    for i, a in enumerate(arrays):
        if i in collect:
            out_shape.append(jax.ShapeDtypeStruct((4, 2, 2, rows[i], 2 * a.shape[1]), jnp.float32))
        else:
            out_shape.append(jax.ShapeDtypeStruct((1, 1, 1, rows[i] // 2, 2 * a.shape[1]), jnp.float32))
    if collect:
        scratch.append(pltpu.SemaphoreType.DMA((m, NUM_DEV)))
    outs = pl.pallas_call(
        functools.partial(reduce_kernel, parts, first, events, n, rows, {i: arrays[i].shape[1] for i in collect}),
        out_shape=out_shape,
        in_specs=[pl.BlockSpec(memory_space=pl.ANY)] * n,
        out_specs=[pl.BlockSpec(memory_space=pl.ANY)] * n,
        scratch_shapes=scratch,
        compiler_params=pltpu.CompilerParams(collective_id=collective_id, has_side_effects=True, vmem_limit_bytes=60 * 2**20),
        name="reduce_blocks",
    )(*ins)
    return [o.reshape(-1, o.shape[-1]) for o in outs]


def exchange_kernel(n_arr, *refs):
    srcs, dsts = refs[:n_arr], refs[n_arr:2 * n_arr]
    ssem, rsem, lsem = refs[2 * n_arr:]
    me = lax.axis_index(AXIS_NAME)
    entry_barrier()

    def copy(a, step):
        to = (me + step) % NUM_DEV
        return remote(srcs[a].at[pl.ds(to, 1)], dsts[a].at[pl.ds(me, 1)], ssem.at[a, step], rsem.at[a, step], to)

    def local(a):
        return pltpu.make_async_copy(srcs[a].at[pl.ds(me, 1)], dsts[a].at[pl.ds(me, 1)], lsem.at[a])

    def start(step, carry):
        for a in range(n_arr):
            copy(a, step).start()
        return carry

    lax.fori_loop(1, NUM_DEV, start, 0)
    for a in range(n_arr):
        local(a).start()

    def finish(step, carry):
        for a in range(n_arr):
            copy(a, step).wait()
        return carry

    lax.fori_loop(1, NUM_DEV, finish, 0)
    for a in range(n_arr):
        local(a).wait()


def exchange(blocks, collective_id):
    n = len(blocks)
    specs = [pl.BlockSpec(memory_space=pl.ANY)] * n
    return pl.pallas_call(
        functools.partial(exchange_kernel, n),
        out_shape=[jax.ShapeDtypeStruct(b.shape, b.dtype) for b in blocks],
        in_specs=specs, out_specs=specs,
        scratch_shapes=[pltpu.SemaphoreType.DMA((n, NUM_DEV)), pltpu.SemaphoreType.DMA((n, NUM_DEV)),
                        pltpu.SemaphoreType.DMA((n,))],
        compiler_params=pltpu.CompilerParams(collective_id=collective_id, has_side_effects=True),
        name="exchange",
    )(*blocks)


BLOCK = 8
MOST = 4
WIDE_OWNERS = ((1, 2, 4), (2, 4, 3), (4, 9, 2))


def owner_blocks(owner):
    blocks = jnp.ones_like(owner)
    for first, last, n in WIDE_OWNERS:
        blocks = jnp.where((owner >= first) & (owner < last), n, blocks)
    return blocks


def cold_kernel(to_owner, *refs):
    if to_owner:
        src, dst, ssem, rsem, lsem = refs
    else:
        src, rows, dst, row_dst, ssem, rsem, lsem, hsem, gsem = refs
    me = lax.axis_index(AXIS_NAME)
    entry_barrier()

    def copy(step, n):
        to = (me + step) % NUM_DEV
        return remote(src.at[pl.ds(to, 1), pl.ds(0, n)], dst.at[pl.ds(me, 1), pl.ds(0, n)], ssem.at[step], rsem.at[step], to)

    def hand(to):
        return remote(rows.at[pl.ds(to, 1)], row_dst, hsem.at[to], gsem.at[0], to)

    def by_size(owner, do):
        wide = owner < 0
        for first, last, n in WIDE_OWNERS:
            hit = (owner >= first) & (owner < last)
            wide = wide | hit
            pl.when(hit)(functools.partial(do, n))
        pl.when(jnp.logical_not(wide))(functools.partial(do, 1))

    def start(step, carry):
        by_size((me + step) % NUM_DEV if to_owner else me, lambda n: copy(step, n).start())
        return carry

    def finish(step, carry):
        by_size((me + step) % NUM_DEV if to_owner else me, lambda n: copy(step, n).wait_send())
        by_size(me if to_owner else (me - step + NUM_DEV) % NUM_DEV, lambda n: copy(step, n).wait_recv())
        return carry

    def each(do):
        def body(to, carry):
            do(hand(to))
            return carry

        lax.fori_loop(1, NUM_DEV, body, 0)

    local = pltpu.make_async_copy(src.at[pl.ds(me, 1)], dst.at[pl.ds(me, 1)], lsem)
    lax.fori_loop(1, NUM_DEV, start, 0)
    local.start()
    if not to_owner:
        @pl.when(me == 0)
        def _():
            each(lambda c: c.start())
            mine = pltpu.make_async_copy(rows.at[pl.ds(0, 1)], row_dst, gsem.at[1])
            mine.start()
            mine.wait()

    lax.fori_loop(1, NUM_DEV, finish, 0)
    local.wait()
    if not to_owner:
        @pl.when(me == 0)
        def _():
            each(lambda c: c.wait_send())

        @pl.when(me != 0)
        def _():
            hand(0).wait_recv()


def cold_exchange(arrays, collective_id):
    to_owner = len(arrays) == 1
    specs = [pl.BlockSpec(memory_space=pl.ANY)] * len(arrays)
    sems = [pltpu.SemaphoreType.DMA((NUM_DEV,)), pltpu.SemaphoreType.DMA((NUM_DEV,)), pltpu.SemaphoreType.DMA]
    out_shape = [jax.ShapeDtypeStruct(arrays[0].shape, arrays[0].dtype)]
    if not to_owner:
        out_shape.append(jax.ShapeDtypeStruct((1, *arrays[1].shape[1:]), arrays[1].dtype))
        sems += [pltpu.SemaphoreType.DMA((NUM_DEV,)), pltpu.SemaphoreType.DMA((2,))]
    return pl.pallas_call(
        functools.partial(cold_kernel, to_owner),
        out_shape=out_shape, in_specs=specs, out_specs=specs, scratch_shapes=sems,
        compiler_params=pltpu.CompilerParams(collective_id=collective_id, has_side_effects=True),
        name="cold_to_owner" if to_owner else "cold_to_device",
    )(*arrays)


CAP = BLOCK * MOST


def add_kernel(fresh, ids, first, count, base, acc, rows, out, buf, sem, asem):
    def get(d, g):
        return pltpu.make_async_copy(rows.at[d, g], buf.at[d, g], sem.at[d, g])

    def each(do):
        def device(d, carry):
            def group(g, inner):
                do(d, g)
                return inner

            return lax.fori_loop(0, (count[d] + BLOCK - 1) // BLOCK, group, carry)

        lax.fori_loop(0, NUM_DEV, device, 0)

    each(lambda d, g: get(d, g).start())
    def fill():
        copy = pltpu.make_async_copy(acc.at[pl.ds(0, out.shape[0])], out, asem.at[0])
        copy.start()
        copy.wait()

    if fresh:
        pl.when(base[0] == 0)(fill)

        @pl.when(base[0] != 0)
        def _():
            def zero(t, carry):
                out[pl.ds(pl.multiple_of(t * 8, 8), 8), :] = jnp.zeros((8, out.shape[1]), jnp.float32)
                return carry

            lax.fori_loop(0, out.shape[0] // 8, zero, 0)
    else:
        fill()

    def add(d, g):
        get(d, g).wait()

        def row(r, carry):
            at = jnp.clip(ids[d, first[d] + BLOCK * g + r] - base[0], 0, out.shape[0] - 1)
            out[pl.ds(at, 1), :] += buf[d, g, pl.ds(r, 1), :]
            return carry

        lax.fori_loop(0, jnp.minimum(count[d] - BLOCK * g, BLOCK), row, 0)

    each(add)


def add_rows(fresh, n_out, ids, first, count, base, acc, rows):
    any_spec = pl.BlockSpec(memory_space=pl.ANY)
    return pl.pallas_call(
        functools.partial(add_kernel, fresh),
        out_shape=jax.ShapeDtypeStruct((n_out, acc.shape[1]), jnp.float32),
        grid_spec=pltpu.PrefetchScalarGridSpec(
            num_scalar_prefetch=4, grid=(1,),
            in_specs=[any_spec, any_spec],
            out_specs=pl.BlockSpec((n_out, acc.shape[1]), lambda i, *_: (0, 0)),
            scratch_shapes=[pltpu.VMEM((NUM_DEV, MOST, BLOCK, acc.shape[1]), jnp.float32),
                            pltpu.SemaphoreType.DMA((NUM_DEV, MOST)), pltpu.SemaphoreType.DMA((1,))]),
        compiler_params=pltpu.CompilerParams(vmem_limit_bytes=40 * 2**20),
        name="add_rows",
    )(ids, first, count, base, acc, rows)


def make_plan(parts, started, awaited):
    begin, cuts = {}, []
    for arr, tiles, order in parts:
        cuts.append((arr, begin.get(arr, 0), 128 * tiles, order))
        begin[arr] = begin.get(arr, 0) + 128 * tiles
    first = [ord(p) - ord("a") for p in started]
    at = [0 if i in first else -1 for i in range(len(parts))]
    events = []
    for letter in awaited:
        i = ord(letter) - ord("a")
        events.append((i, at[i]))
        at[i] += 1
    return cuts, first, events


GATHER_PLAN = make_plan(
    ((0, 8, 'zxy'),
     (0, 8, 'zyx'),
     (1, 4, 'zxy'),
     (1, 12, 'yzx'),
     (2, 7, 'yxz'),
     (2, 7, 'zxy'),
     (2, 2, 'yxz'),
     (3, 16, 'xzy')),
    "adbcfeg", "ebfgcbcabfcafdecadhbfhdhcgadhghegefgbadeh")
REDUCE_PLAN = make_plan(
    ((3, 4, 'yxz'),
     (3, 4, 'xyz'),
     (0, 3, 'xzy'),
     (0, 2, 'yxz'),
     (0, 3, 'yxz'),
     (1, 4, 'yxz'),
     (1, 1, 'zxy'),
     (1, 3, 'yxz'),
     (2, 1, 'xzy'),
     (2, 5, 'zyx'),
     (2, 2, 'xyz')),
    "adefhbigcjk", "gabjgdcijgecikadjgcfiadeciadeafdhefbefhbkfhbjkghcibjkhk")
HOT_ROWS = 1024


def norm_forward(x_rows, gain_full):
    inv_rms = lax.rsqrt(jnp.mean(x_rows * x_rows, axis=-1, keepdims=True) + 1e-5)
    h_rows = x_rows * inv_rms
    return inv_rms, h_rows, (h_rows * gain_full).astype(jnp.bfloat16)


def dot(a, b, dims, precision=None):
    return lax.dot_general(a, b, (dims, ((), ())), preferred_element_type=jnp.float32, precision=precision)


def solution(mesh):
    def local_step(tokens, embed_shard, gain_shard, wq_shard, wk_shard, wv_shard, d_query, d_key, d_value):
        vocab_local, width = embed_shard.shape
        n_tok = tokens.shape[1]
        me = lax.axis_index(AXIS_NAME)
        core = me % 2
        swap = [(d, d ^ 1) for d in range(NUM_DEV)]
        half = width // 2

        def partner(a):
            return lax.ppermute(a, AXIS_NAME, swap)

        def my_half(a, c):
            return lax.dynamic_slice_in_dim(a, c * half, half, axis=1)

        def paired(a):
            return jnp.concatenate([my_half(a, core), partner(my_half(a, 1 - core))], axis=0)

        tok = tokens[0]
        pos = jnp.arange(n_tok, dtype=jnp.int32)
        before = (tok[None, :] < tok[:, None]) | ((tok[None, :] == tok[:, None]) & (pos[None, :] < pos[:, None]))
        rank = jnp.sum(before.astype(jnp.int32), axis=1)
        place = rank[None, :] == pos[:, None]
        sorted_ids = jnp.sum(jnp.where(place, tok[None, :], 0), axis=1)

        hot_own = jnp.pad(embed_shard.astype(jnp.bfloat16), ((0, HOT_ROWS - vocab_local), (0, 0)))
        gain_rows = gain_shard.shape[0]
        ids_all, gains = exchange(
            [jnp.broadcast_to(sorted_ids.reshape(1, 2, 128), (NUM_DEV, 2, 128)),
             jnp.broadcast_to(jnp.pad(gain_shard, (0, 128 - gain_rows)), (NUM_DEV, 1, 128))], 4)
        gain_full = gains[:, 0, :gain_rows].reshape(-1)
        ids_all = ids_all.reshape(NUM_DEV, n_tok)
        limits = vocab_local * jnp.arange(NUM_DEV + 1, dtype=jnp.int32)
        starts = jnp.sum((ids_all[:, :, None] < limits).astype(jnp.int32), axis=1)
        counts = (starts[:, 1:] - starts[:, :-1]).at[:, 0].set(0)
        owner_first = lax.dynamic_index_in_dim(starts, me, axis=1, keepdims=False)
        owner_count = lax.dynamic_index_in_dim(counts, me, axis=1, keepdims=False)
        my_first = lax.dynamic_index_in_dim(starts, me, axis=0, keepdims=False)[:NUM_DEV]
        my_count = lax.dynamic_index_in_dim(counts, me, axis=0, keepdims=False)
        base = (me * vocab_local).reshape(1)
        owners = jnp.arange(NUM_DEV, dtype=jnp.int32)
        slot = jnp.arange(CAP, dtype=jnp.int32)
        caps = BLOCK * owner_blocks(owners)
        my_cap = BLOCK * owner_blocks(me)
        rounds = jnp.maximum(jnp.max((counts + caps - 1) // caps), 1)
        tok_owner = tok // vocab_local
        tok_slot = rank - jnp.sum(jnp.where(tok_owner[:, None] == owners, my_first, 0), axis=1)
        tok_cap = BLOCK * owner_blocks(tok_owner)

        def cold_round(carry):
            step, cold, _ = carry
            want = owner_first[:, None] + step * my_cap + slot
            ids = jnp.sum(jnp.where(want[:, :, None] == pos, ids_all[:, None, :], 0), axis=2) - base
            pick = (ids.reshape(-1, 1) == jnp.arange(HOT_ROWS, dtype=jnp.int32)).astype(jnp.bfloat16)
            rows = dot(pick, hot_own, ((1,), (0,))).astype(jnp.bfloat16)
            got, handed = cold_exchange([rows.reshape(NUM_DEV, MOST, BLOCK, width), hot_blocks], 6)
            at = tok_slot - step * tok_cap
            here = (tok_owner > 0) & (at >= 0) & (at < tok_cap)
            mine = jnp.take(got.reshape(-1, width), jnp.where(here, tok_owner * CAP + at, 0), axis=0)
            return step + 1, jnp.where(here[:, None], mine, cold), handed

        hot_blocks = hot_own.reshape(NUM_DEV, HOT_ROWS // NUM_DEV, width)
        carry = cold_round((jnp.int32(0), jnp.zeros((n_tok, width), jnp.bfloat16), None))
        _, cold, handed = lax.while_loop(lambda carry: carry[0] < rounds, cold_round, carry)

        shards = [w.astype(jnp.bfloat16) for w in (wq_shard, wk_shard, wv_shard)]
        wq_full, wk_full, wv_full, hot = all_gather_blocks([*shards, handed[0]], GATHER_PLAN, 1)

        hot_sel = ((tok[:, None] == jnp.arange(HOT_ROWS, dtype=jnp.int32)) & (tok[:, None] < vocab_local)).astype(jnp.bfloat16)
        x_rows = dot(hot_sel, hot, ((1,), (0,))) + cold.astype(jnp.float32)
        inv_rms, h_rows, normed = norm_forward(x_rows, gain_full)
        dq, dk, dv = d_query[0], d_key[0], d_value[0]
        normed_pair = jnp.concatenate([normed, partner(normed)], axis=0)
        d_w = [dot(normed_pair, paired(d), ((0,), (0,))) for d in (dq, dk, dv)]
        query_proj, key_proj, value_proj = [dot(normed, w, ((1,), (0,))).astype(jnp.bfloat16)[None]
                                            for w in (wq_full, wk_full, wv_full)]
        d_normed = (dot(dq, wq_full, ((1,), (1,))) + dot(dk, wk_full, ((1,), (1,))) + dot(dv, wv_full, ((1,), (1,))))
        gain_part = jnp.sum(d_normed * h_rows, axis=0)
        u_rows = d_normed * gain_full
        d_x = inv_rms * (u_rows - h_rows * jnp.mean(u_rows * h_rows, axis=-1, keepdims=True))

        pair_ids = jnp.concatenate([tok, partner(tok)])
        pair_sel = ((pair_ids[:, None] == jnp.arange(HOT_ROWS, dtype=jnp.int32)) & (pair_ids[:, None] < vocab_local)).astype(jnp.float32)
        hot_part = dot(pair_sel, paired(d_x), ((0,), (0,)), lax.Precision.HIGHEST)
        d_w_query, d_w_key, d_w_value, hot_sum = reduce_scatter_blocks([*d_w, hot_part], REDUCE_PLAN, (3,), 2)

        gain_blocks = jnp.pad(gain_part.reshape(NUM_DEV, 1, -1), ((0, 0), (0, 0), (0, 128 - gain_rows)))
        d_norm_gain = jnp.sum(exchange([gain_blocks], 5)[0], axis=(0, 1))[:gain_rows]
        def add_round(step, total, fresh):
            want = my_first[:, None] + step * caps[:, None] + slot
            src = jnp.sum(jnp.where(want[:, :, None] == rank, pos, 0), axis=2)
            rows = jnp.take(d_x, src.reshape(-1), axis=0).reshape(NUM_DEV, MOST, BLOCK, width)
            got = cold_exchange([rows], 7)[0]
            left = jnp.clip(owner_count - step * my_cap, 0, my_cap)
            return add_rows(fresh, vocab_local, ids_all, owner_first + step * my_cap, left, base, total, got)

        _, d_embed = lax.while_loop(lambda carry: carry[0] < rounds,
                                    lambda carry: (carry[0] + 1, add_round(*carry, False)),
                                    (jnp.int32(1), add_round(jnp.int32(0), hot_sum, True)))
        return (query_proj, key_proj, value_proj, d_embed, d_norm_gain, d_w_query, d_w_key, d_w_value)

    row_spec = P(AXIS_NAME, None)
    act_spec = P(AXIS_NAME, None, None)
    vec_spec = P(AXIS_NAME)
    return jax.shard_map(local_step, mesh=mesh,
                         in_specs=(row_spec, row_spec, vec_spec, row_spec, row_spec, row_spec, act_spec, act_spec, act_spec),
                         out_specs=(act_spec, act_spec, act_spec, row_spec, vec_spec, row_spec, row_spec, row_spec),
                         check_vma=False)
```

```python
import functools
import jax
import jax.numpy as jnp
from jax import lax
from jax.experimental import pallas as pl
from jax.experimental.pallas import tpu as pltpu
from jax.sharding import PartitionSpec as P

AXIS_NAME = "fsdp"
NUM_DEV = 32
DIM_SIZE = {"z": 4, "y": 2, "x": 2}


def coords():
    me = lax.axis_index(AXIS_NAME)
    return me // 8, (me // 4) % 2, (me // 2) % 2, me % 2


def dev_at(z, y, x, c):
    return ((z * 2 + y) * 2 + x) * 2 + c


def neighbour(dim):
    z, y, x, c = coords()
    if dim == "z":
        return dev_at((z + 1) % 4, y, x, c)
    if dim == "y":
        return dev_at(z, 1 - y, x, c)
    if dim == "x":
        return dev_at(z, y, 1 - x, c)
    return dev_at(z, y, x, 1 - c)


def entry_barrier():
    me = lax.axis_index(AXIS_NAME)
    barrier = pltpu.get_barrier_semaphore()

    def signal(step, carry):
        pl.semaphore_signal(barrier, inc=1, device_id=((me + step) % NUM_DEV,), device_id_type=pl.DeviceIdType.MESH)
        return carry

    lax.fori_loop(1, NUM_DEV, signal, 0)
    pl.semaphore_wait(barrier, NUM_DEV - 1)


def remote(src, dst, send_sem, recv_sem, dev):
    return pltpu.make_async_remote_copy(src_ref=src, dst_ref=dst, send_sem=send_sem, recv_sem=recv_sem,
                                        device_id=(dev,), device_id_type=pl.DeviceIdType.MESH)


def gather_steps(order):
    steps, whole = [], []
    for dim in order:
        for ring in range(DIM_SIZE[dim] - 1):
            steps.append((dim, ring, tuple(whole)))
        whole.append(dim)
    return steps


def box(dim, ring, whole, shift):
    z, y, x, _ = coords()
    pos = {"z": z, "y": y, "x": x}
    idx = []
    for d in ("z", "y", "x"):
        if d == dim:
            at = (pos[d] + 2 * DIM_SIZE[d] - ring - shift) % DIM_SIZE[d]
            idx.append(pl.ds(at, 1))
        elif d in whole:
            idx.append(pl.ds(0, DIM_SIZE[d]))
        else:
            idx.append(pl.ds(pos[d], 1))
    return tuple(idx)


def gather_kernel(parts, first, events, n_arr, *refs):
    ins, outs = refs[:n_arr], refs[n_arr:2 * n_arr]
    ssem, rsem, csem, dsem, lsem = refs[2 * n_arr:]
    z, y, x, c = coords()
    me = lax.axis_index(AXIS_NAME)
    here = (pl.ds(z, 1), pl.ds(y, 1), pl.ds(x, 1))
    entry_barrier()
    partner = neighbour("c")

    def cut(arr, idx, core, part):
        _, col, ncol, _ = part
        return outs[arr].at[idx[0], idx[1], idx[2], pl.ds(core, 1), :, pl.ds(col, ncol)]

    def own(part):
        return ins[part[0]].at[:, :, :, :, :, pl.ds(part[1], part[2])]

    steps = [gather_steps(p[3]) for p in parts]

    def hop(i, k):
        dim, ring, whole = steps[i][k]
        idx = box(dim, ring, whole, 0)
        src = own(parts[i]) if k == 0 else cut(parts[i][0], idx, c, parts[i])
        return remote(src, cut(parts[i][0], idx, c, parts[i]), ssem.at[i, k], rsem.at[i, k], neighbour(dim))

    def cross(i, k):
        if k < 0:
            idx, src = here, own(parts[i])
        else:
            idx = box(*steps[i][k], 1)
            src = cut(parts[i][0], idx, c, parts[i])
        return remote(src, cut(parts[i][0], idx, c, parts[i]), csem.at[i, k + 1], dsem.at[i, k + 1], partner)

    def local(i):
        return pltpu.make_async_copy(own(parts[i]), cut(parts[i][0], here, c, parts[i]), lsem.at[i])

    for i in first:
        hop(i, 0).start()
    for i in first:
        local(i).start()
        cross(i, -1).start()
    for i in first:
        local(i).wait()
    for i, k in events:
        if k < 0:
            hop(i, 0).start()
            local(i).start()
            cross(i, -1).start()
            local(i).wait()
            continue
        hop(i, k).wait_recv()
        if k + 1 < len(steps[i]):
            hop(i, k + 1).start()
        cross(i, k).start()
    for i in range(len(parts)):
        for k in range(-1, len(steps[i])):
            cross(i, k).wait()
        for k in range(len(steps[i])):
            hop(i, k).wait_send()


def all_gather_blocks(blocks, plan, collective_id):
    parts, first, events = plan
    n, m = len(blocks), len(parts)
    outs = pl.pallas_call(
        functools.partial(gather_kernel, parts, first, events, n),
        out_shape=[jax.ShapeDtypeStruct((4, 2, 2, 2, *b.shape), b.dtype) for b in blocks],
        in_specs=[pl.BlockSpec(memory_space=pltpu.VMEM)] * n,
        out_specs=[pl.BlockSpec(memory_space=pl.ANY)] * n,
        scratch_shapes=[pltpu.SemaphoreType.DMA((m, 5)), pltpu.SemaphoreType.DMA((m, 5)),
                        pltpu.SemaphoreType.DMA((m, 6)), pltpu.SemaphoreType.DMA((m, 6)), pltpu.SemaphoreType.DMA((m,))],
        compiler_params=pltpu.CompilerParams(collective_id=collective_id, has_side_effects=True),
        name="gather_blocks",
    )(*[b.reshape(1, 1, 1, 1, *b.shape) for b in blocks])
    return [o.reshape(NUM_DEV * b.shape[0], b.shape[1]) for o, b in zip(outs, blocks)]


def add_into(dst, src, rows):
    lead = dst.shape[:-2]
    count = 1
    for n in lead:
        count *= n
    step = 8
    per = rows // step

    def body(t, carry):
        blk, off = t // per, pl.multiple_of((t % per) * step, step)
        idx = []
        for n in reversed(lead):
            idx.append(blk % n)
            blk = blk // n
        at = (*reversed(idx), pl.ds(off, step), slice(None))
        dst[at] = dst[at] + src[at]
        return carry

    lax.fori_loop(0, count * per, body, 0)


def scatter_steps(order):
    steps, done = [], []
    for dim in order:
        for ring in range(DIM_SIZE[dim] - 1):
            steps.append((dim, ring, tuple(done)))
        done.append(dim)
    return steps


def left_shape(done):
    return tuple(1 if d in done else DIM_SIZE[d] for d in ("z", "y", "x"))


def reduce_kernel(parts, first_hops, events, n_arr, rows, collect, *refs):
    ins, outs = refs[:n_arr], refs[n_arr + 1:2 * n_arr + 1]
    cold_src, cold_dst = refs[n_arr], refs[2 * n_arr + 1]
    cold_ssem, cold_rsem, cold_lsem = refs[-3:]
    cold_start, cold_finish = cold_copies(True, cold_src, cold_dst, cold_ssem, cold_rsem)
    rest = refs[2 * n_arr + 2:-3]
    n_part = len(parts)
    recv = []
    at = 0
    for p in parts:
        recv.append(rest[at:at + 5])
        at += 5
    own_buf = []
    for p in parts:
        n_own = DIM_SIZE[p[3][0]] - 1
        own_buf.append(rest[at:at + n_own])
        at += n_own
    ssem, rsem, lsem, osem, tsem, usem = rest[at:at + 6]
    gsem = rest[at + 6] if collect else None
    z, y, x, c = coords()
    me = lax.axis_index(AXIS_NAME)
    pos = {"z": z, "y": y, "x": x}
    steps = [scatter_steps(p[3]) for p in parts]

    def pick(ref, dim, index):
        sel = [pl.ds(index, 1) if d == dim else slice(None) for d in ("z", "y", "x")]
        return ref.at[sel[0], sel[1], sel[2]]

    def first(i, dim, index):
        arr, col, ncol, _ = parts[i]
        sel = [pl.ds(index, 1) if d == dim else slice(None) for d in ("z", "y", "x")]
        return ins[arr].at[sel[0], sel[1], sel[2], :, pl.ds(col, ncol)]

    def held(i, dim, index, k):
        return first(i, dim, index) if k == 0 else pick(recv[i][k - 1], dim, index)

    def keep_index(dim, ring):
        n = DIM_SIZE[dim]
        return (pos[dim] + 2 * n - ring - 2) % n if n > 2 else pos[dim]

    def hop(i, k):
        dim, ring, _ = steps[i][k]
        n = DIM_SIZE[dim]
        if ring == 0:
            src = held(i, dim, (pos[dim] + n - 1) % n, k)
        else:
            src = recv[i][k - 1]
        return remote(src, recv[i][k], ssem.at[i, k], rsem.at[i, k], neighbour(dim))

    def load(i, k):
        dim, ring, _ = steps[i][k]
        return pltpu.make_async_copy(first(i, dim, keep_index(dim, ring)), own_buf[i][k], lsem.at[i, k])

    entry_barrier()
    for i in first_hops:
        hop(i, 0).start()
    for i in first_hops:
        for k in range(len(own_buf[i])):
            load(i, k).start()

    def finish(i):
        arr, col, ncol, _ = parts[i]
        acc = recv[i][4]
        r = rows[arr]
        if arr in collect:
            idx = (pl.ds(z, 1), pl.ds(y, 1), pl.ds(x, 1), slice(None), pl.ds(c * collect[arr] + col, ncol))
            dst = outs[arr].at[idx]

            @pl.when(me != 0)
            def _():
                remote(acc, dst, tsem.at[i], gsem.at[i, me], 0).start()

            @pl.when(me == 0)
            def _():
                pltpu.make_async_copy(acc, dst, osem.at[i]).start()
            return
        half = r // 2
        cols = pl.ds(c * (outs[arr].shape[-1] // 2) + col, ncol)
        dst = outs[arr].at[:, :, :, :, cols]
        mine = acc.at[:, :, :, pl.ds(c * half, half), :]
        theirs = acc.at[:, :, :, pl.ds((1 - c) * half, half), :]
        remote(theirs, dst, tsem.at[i], usem.at[i], neighbour("c")).start()
        pltpu.make_async_copy(mine, dst, osem.at[i]).start()

    def finish_wait(i):
        arr, col, ncol, _ = parts[i]
        acc = recv[i][4]
        r = rows[arr]
        if arr in collect:
            dst = outs[arr].at[pl.ds(z, 1), pl.ds(y, 1), pl.ds(x, 1), :, pl.ds(c * collect[arr] + col, ncol)]

            @pl.when(me != 0)
            def _():
                remote(acc, dst, tsem.at[i], gsem.at[i, me], 0).wait_send()

            @pl.when(me == 0)
            def _():
                pltpu.make_async_copy(acc, dst, osem.at[i]).wait()

                def one(s, carry):
                    from_at = outs[arr].at[pl.ds(s // 8, 1), pl.ds((s // 4) % 2, 1), pl.ds((s // 2) % 2, 1), :,
                                           pl.ds(pl.multiple_of((s % 2) * collect[arr] + col, 128), ncol)]
                    remote(acc, from_at, tsem.at[i], gsem.at[i, s], 0).wait_recv()
                    return carry

                lax.fori_loop(1, NUM_DEV, one, 0)
            return
        half = r // 2
        cols = pl.ds(c * (outs[arr].shape[-1] // 2) + col, ncol)
        dst = outs[arr].at[:, :, :, :, cols]
        mine = acc.at[:, :, :, pl.ds(c * half, half), :]
        theirs = acc.at[:, :, :, pl.ds((1 - c) * half, half), :]
        remote(theirs, dst, tsem.at[i], usem.at[i], neighbour("c")).wait()
        pltpu.make_async_copy(mine, dst, osem.at[i]).wait()

    for turn, (i, k) in enumerate(events):
        if turn == COLD_TURN:
            lax.fori_loop(1, NUM_DEV, cold_start, 0)
            pltpu.make_async_copy(cold_src.at[pl.ds(me, 1)], cold_dst.at[pl.ds(me, 1)], cold_lsem).start()
        dim, ring, _ = steps[i][k]
        start = k - ring
        hop(i, k).wait_recv()
        if k < len(own_buf[i]):
            load(i, k).wait()
            src = own_buf[i][k]
        else:
            src = held(i, dim, keep_index(dim, ring), start)
        add_into(recv[i][k], src, rows[parts[i][0]])
        if k + 1 < 5:
            hop(i, k + 1).start()
        else:
            finish(i)
    for i in range(n_part):
        for k in range(5):
            hop(i, k).wait_send()
        finish_wait(i)
    lax.fori_loop(1, NUM_DEV, cold_finish, 0)
    pltpu.make_async_copy(cold_src.at[pl.ds(me, 1)], cold_dst.at[pl.ds(me, 1)], cold_lsem).wait()


def reduce_scatter_blocks(arrays, cold, plan, collect, collective_id):
    parts, first, events = plan
    n = len(arrays)
    rows = [a.shape[0] // 16 for a in arrays]
    ins = [a.reshape(4, 2, 2, r, a.shape[1]) for a, r in zip(arrays, rows)]
    scratch = []
    for p in parts:
        for dim, ring, done in scatter_steps(p[3]):
            scratch.append(pltpu.VMEM((*left_shape(done + (dim,)), rows[p[0]], p[2]), jnp.float32))
    for p in parts:
        for k in range(DIM_SIZE[p[3][0]] - 1):
            scratch.append(pltpu.VMEM((*left_shape((p[3][0],)), rows[p[0]], p[2]), jnp.float32))
    m = len(parts)
    scratch += [pltpu.SemaphoreType.DMA((m, 5)), pltpu.SemaphoreType.DMA((m, 5)), pltpu.SemaphoreType.DMA((m, 3)),
                pltpu.SemaphoreType.DMA((m,)), pltpu.SemaphoreType.DMA((m,)), pltpu.SemaphoreType.DMA((m,))]
    out_shape = []
    for i, a in enumerate(arrays):
        if i in collect:
            out_shape.append(jax.ShapeDtypeStruct((4, 2, 2, rows[i], 2 * a.shape[1]), jnp.float32))
        else:
            out_shape.append(jax.ShapeDtypeStruct((1, 1, 1, rows[i] // 2, 2 * a.shape[1]), jnp.float32))
    if collect:
        scratch.append(pltpu.SemaphoreType.DMA((m, NUM_DEV)))
    scratch += [pltpu.SemaphoreType.DMA((NUM_DEV,)), pltpu.SemaphoreType.DMA((NUM_DEV,)), pltpu.SemaphoreType.DMA]
    out_shape.append(jax.ShapeDtypeStruct(cold.shape, cold.dtype))
    outs = pl.pallas_call(
        functools.partial(reduce_kernel, parts, first, events, n, rows, {i: arrays[i].shape[1] for i in collect}),
        out_shape=out_shape,
        in_specs=[pl.BlockSpec(memory_space=pl.ANY)] * (n + 1),
        out_specs=[pl.BlockSpec(memory_space=pl.ANY)] * (n + 1),
        scratch_shapes=scratch,
        compiler_params=pltpu.CompilerParams(collective_id=collective_id, has_side_effects=True, vmem_limit_bytes=60 * 2**20),
        name="reduce_blocks",
    )(*ins, cold)
    return [o.reshape(-1, o.shape[-1]) for o in outs[:-1]] + [outs[-1]]


def exchange_kernel(n_arr, *refs):
    srcs, dsts = refs[:n_arr], refs[n_arr:2 * n_arr]
    ssem, rsem, lsem = refs[2 * n_arr:]
    me = lax.axis_index(AXIS_NAME)
    entry_barrier()

    def copy(a, step):
        to = (me + step) % NUM_DEV
        return remote(srcs[a].at[pl.ds(to, 1)], dsts[a].at[pl.ds(me, 1)], ssem.at[a, step], rsem.at[a, step], to)

    def local(a):
        return pltpu.make_async_copy(srcs[a].at[pl.ds(me, 1)], dsts[a].at[pl.ds(me, 1)], lsem.at[a])

    def start(step, carry):
        for a in range(n_arr):
            copy(a, step).start()
        return carry

    lax.fori_loop(1, NUM_DEV, start, 0)
    for a in range(n_arr):
        local(a).start()

    def finish(step, carry):
        for a in range(n_arr):
            copy(a, step).wait()
        return carry

    lax.fori_loop(1, NUM_DEV, finish, 0)
    for a in range(n_arr):
        local(a).wait()


def exchange(blocks, collective_id):
    n = len(blocks)
    specs = [pl.BlockSpec(memory_space=pl.ANY)] * n
    return pl.pallas_call(
        functools.partial(exchange_kernel, n),
        out_shape=[jax.ShapeDtypeStruct(b.shape, b.dtype) for b in blocks],
        in_specs=specs, out_specs=specs,
        scratch_shapes=[pltpu.SemaphoreType.DMA((n, NUM_DEV)), pltpu.SemaphoreType.DMA((n, NUM_DEV)),
                        pltpu.SemaphoreType.DMA((n,))],
        compiler_params=pltpu.CompilerParams(collective_id=collective_id, has_side_effects=True),
        name="exchange",
    )(*blocks)


BLOCK = 8
MOST = 4
WIDE_OWNERS = ((1, 2, 4), (2, 4, 3), (4, 9, 2))


def owner_blocks(owner):
    blocks = jnp.ones_like(owner)
    for first, last, n in WIDE_OWNERS:
        blocks = jnp.where((owner >= first) & (owner < last), n, blocks)
    return blocks


def cold_copies(to_owner, src, dst, ssem, rsem):
    me = lax.axis_index(AXIS_NAME)

    def copy(step, n):
        to = (me + step) % NUM_DEV
        return remote(src.at[pl.ds(to, 1), pl.ds(0, n)], dst.at[pl.ds(me, 1), pl.ds(0, n)], ssem.at[step], rsem.at[step], to)

    def by_size(owner, do):
        wide = owner < 0
        for first, last, n in WIDE_OWNERS:
            hit = (owner >= first) & (owner < last)
            wide = wide | hit
            pl.when(hit)(functools.partial(do, n))
        pl.when(jnp.logical_not(wide))(functools.partial(do, 1))

    def start(step, carry):
        by_size((me + step) % NUM_DEV if to_owner else me, lambda n: copy(step, n).start())
        return carry

    def finish(step, carry):
        by_size((me + step) % NUM_DEV if to_owner else me, lambda n: copy(step, n).wait_send())
        by_size(me if to_owner else (me - step + NUM_DEV) % NUM_DEV, lambda n: copy(step, n).wait_recv())
        return carry

    return start, finish


def cold_kernel(to_owner, *refs):
    if to_owner:
        src, dst, ssem, rsem, lsem = refs
    else:
        src, rows, dst, row_dst, ssem, rsem, lsem, hsem, gsem = refs
    me = lax.axis_index(AXIS_NAME)
    entry_barrier()

    start, finish = cold_copies(to_owner, src, dst, ssem, rsem)

    def hand(to):
        return remote(rows.at[pl.ds(to, 1)], row_dst, hsem.at[to], gsem.at[0], to)

    def each(do):
        def body(to, carry):
            do(hand(to))
            return carry

        lax.fori_loop(1, NUM_DEV, body, 0)

    local = pltpu.make_async_copy(src.at[pl.ds(me, 1)], dst.at[pl.ds(me, 1)], lsem)
    lax.fori_loop(1, NUM_DEV, start, 0)
    local.start()
    if not to_owner:
        @pl.when(me == 0)
        def _():
            each(lambda c: c.start())
            mine = pltpu.make_async_copy(rows.at[pl.ds(0, 1)], row_dst, gsem.at[1])
            mine.start()
            mine.wait()

    lax.fori_loop(1, NUM_DEV, finish, 0)
    local.wait()
    if not to_owner:
        @pl.when(me == 0)
        def _():
            each(lambda c: c.wait_send())

        @pl.when(me != 0)
        def _():
            hand(0).wait_recv()


def cold_exchange(arrays, collective_id):
    to_owner = len(arrays) == 1
    specs = [pl.BlockSpec(memory_space=pl.ANY)] * len(arrays)
    sems = [pltpu.SemaphoreType.DMA((NUM_DEV,)), pltpu.SemaphoreType.DMA((NUM_DEV,)), pltpu.SemaphoreType.DMA]
    out_shape = [jax.ShapeDtypeStruct(arrays[0].shape, arrays[0].dtype)]
    if not to_owner:
        out_shape.append(jax.ShapeDtypeStruct((1, *arrays[1].shape[1:]), arrays[1].dtype))
        sems += [pltpu.SemaphoreType.DMA((NUM_DEV,)), pltpu.SemaphoreType.DMA((2,))]
    return pl.pallas_call(
        functools.partial(cold_kernel, to_owner),
        out_shape=out_shape, in_specs=specs, out_specs=specs, scratch_shapes=sems,
        compiler_params=pltpu.CompilerParams(collective_id=collective_id, has_side_effects=True),
        name="cold_to_owner" if to_owner else "cold_to_device",
    )(*arrays)


CAP = BLOCK * MOST


def add_kernel(fresh, ids, first, count, base, acc, rows, out, buf, sem, asem):
    def get(d, g):
        return pltpu.make_async_copy(rows.at[d, g], buf.at[d, g], sem.at[d, g])

    def each(do):
        def device(d, carry):
            def group(g, inner):
                do(d, g)
                return inner

            return lax.fori_loop(0, (count[d] + BLOCK - 1) // BLOCK, group, carry)

        lax.fori_loop(0, NUM_DEV, device, 0)

    each(lambda d, g: get(d, g).start())
    def fill():
        copy = pltpu.make_async_copy(acc.at[pl.ds(0, out.shape[0])], out, asem.at[0])
        copy.start()
        copy.wait()

    if fresh:
        pl.when(base[0] == 0)(fill)

        @pl.when(base[0] != 0)
        def _():
            def zero(t, carry):
                out[pl.ds(pl.multiple_of(t * 8, 8), 8), :] = jnp.zeros((8, out.shape[1]), jnp.float32)
                return carry

            lax.fori_loop(0, out.shape[0] // 8, zero, 0)
    else:
        fill()

    def add(d, g):
        get(d, g).wait()

        def row(r, carry):
            at = jnp.clip(ids[d, first[d] + BLOCK * g + r] - base[0], 0, out.shape[0] - 1)
            out[pl.ds(at, 1), :] += buf[d, g, pl.ds(r, 1), :]
            return carry

        lax.fori_loop(0, jnp.minimum(count[d] - BLOCK * g, BLOCK), row, 0)

    each(add)


def add_rows(fresh, n_out, ids, first, count, base, acc, rows):
    any_spec = pl.BlockSpec(memory_space=pl.ANY)
    return pl.pallas_call(
        functools.partial(add_kernel, fresh),
        out_shape=jax.ShapeDtypeStruct((n_out, acc.shape[1]), jnp.float32),
        grid_spec=pltpu.PrefetchScalarGridSpec(
            num_scalar_prefetch=4, grid=(1,),
            in_specs=[any_spec, any_spec],
            out_specs=pl.BlockSpec((n_out, acc.shape[1]), lambda i, *_: (0, 0)),
            scratch_shapes=[pltpu.VMEM((NUM_DEV, MOST, BLOCK, acc.shape[1]), jnp.float32),
                            pltpu.SemaphoreType.DMA((NUM_DEV, MOST)), pltpu.SemaphoreType.DMA((1,))]),
        compiler_params=pltpu.CompilerParams(vmem_limit_bytes=40 * 2**20),
        name="add_rows",
    )(ids, first, count, base, acc, rows)


def make_plan(parts, started, awaited):
    begin, cuts = {}, []
    for arr, tiles, order in parts:
        cuts.append((arr, begin.get(arr, 0), 128 * tiles, order))
        begin[arr] = begin.get(arr, 0) + 128 * tiles
    first = [ord(p) - ord("a") for p in started]
    at = [0 if i in first else -1 for i in range(len(parts))]
    events = []
    for letter in awaited:
        i = ord(letter) - ord("a")
        events.append((i, at[i]))
        at[i] += 1
    return cuts, first, events


GATHER_PLAN = make_plan(
    ((0, 8, 'zxy'),
     (0, 8, 'zyx'),
     (1, 4, 'zxy'),
     (1, 12, 'yzx'),
     (2, 7, 'yxz'),
     (2, 7, 'zxy'),
     (2, 2, 'yxz'),
     (3, 16, 'xzy')),
    "adbcfeg", "ebfgcbcabfcafdecadhbfhdhcgadhghegefgbadeh")
REDUCE_PLAN = make_plan(
    ((3, 4, 'yxz'),
     (3, 4, 'xyz'),
     (0, 3, 'xzy'),
     (0, 2, 'yxz'),
     (0, 3, 'yxz'),
     (1, 4, 'yxz'),
     (1, 1, 'zxy'),
     (1, 3, 'yxz'),
     (2, 1, 'xzy'),
     (2, 5, 'zyx'),
     (2, 2, 'xyz')),
    "adefhbigcjk", "gabjgdcijgecikadjgcfiadeciadeafdhefbefhbkfhbjkghcibjkhk")
HOT_ROWS = 1024
COLD_TURN = 27


def norm_forward(x_rows, gain_full):
    inv_rms = lax.rsqrt(jnp.mean(x_rows * x_rows, axis=-1, keepdims=True) + 1e-5)
    h_rows = x_rows * inv_rms
    return inv_rms, h_rows, (h_rows * gain_full).astype(jnp.bfloat16)


def dot(a, b, dims, precision=None):
    return lax.dot_general(a, b, (dims, ((), ())), preferred_element_type=jnp.float32, precision=precision)


def solution(mesh):
    def local_step(tokens, embed_shard, gain_shard, wq_shard, wk_shard, wv_shard, d_query, d_key, d_value):
        vocab_local, width = embed_shard.shape
        n_tok = tokens.shape[1]
        me = lax.axis_index(AXIS_NAME)
        core = me % 2
        swap = [(d, d ^ 1) for d in range(NUM_DEV)]
        half = width // 2

        def partner(a):
            return lax.ppermute(a, AXIS_NAME, swap)

        def my_half(a, c):
            return lax.dynamic_slice_in_dim(a, c * half, half, axis=1)

        def paired(a):
            return jnp.concatenate([my_half(a, core), partner(my_half(a, 1 - core))], axis=0)

        tok = tokens[0]
        pos = jnp.arange(n_tok, dtype=jnp.int32)
        before = (tok[None, :] < tok[:, None]) | ((tok[None, :] == tok[:, None]) & (pos[None, :] < pos[:, None]))
        rank = jnp.sum(before.astype(jnp.int32), axis=1)
        place = rank[None, :] == pos[:, None]
        sorted_ids = jnp.sum(jnp.where(place, tok[None, :], 0), axis=1)

        hot_own = jnp.pad(embed_shard.astype(jnp.bfloat16), ((0, HOT_ROWS - vocab_local), (0, 0)))
        gain_rows = gain_shard.shape[0]
        ids_all, gains = exchange(
            [jnp.broadcast_to(sorted_ids.reshape(1, 2, 128), (NUM_DEV, 2, 128)),
             jnp.broadcast_to(jnp.pad(gain_shard, (0, 128 - gain_rows)), (NUM_DEV, 1, 128))], 4)
        gain_full = gains[:, 0, :gain_rows].reshape(-1)
        ids_all = ids_all.reshape(NUM_DEV, n_tok)
        limits = vocab_local * jnp.arange(NUM_DEV + 1, dtype=jnp.int32)
        starts = jnp.sum((ids_all[:, :, None] < limits).astype(jnp.int32), axis=1)
        counts = (starts[:, 1:] - starts[:, :-1]).at[:, 0].set(0)
        owner_first = lax.dynamic_index_in_dim(starts, me, axis=1, keepdims=False)
        owner_count = lax.dynamic_index_in_dim(counts, me, axis=1, keepdims=False)
        my_first = lax.dynamic_index_in_dim(starts, me, axis=0, keepdims=False)[:NUM_DEV]
        my_count = lax.dynamic_index_in_dim(counts, me, axis=0, keepdims=False)
        base = (me * vocab_local).reshape(1)
        owners = jnp.arange(NUM_DEV, dtype=jnp.int32)
        slot = jnp.arange(CAP, dtype=jnp.int32)
        caps = BLOCK * owner_blocks(owners)
        my_cap = BLOCK * owner_blocks(me)
        rounds = jnp.maximum(jnp.max((counts + caps - 1) // caps), 1)
        tok_owner = tok // vocab_local
        tok_slot = rank - jnp.sum(jnp.where(tok_owner[:, None] == owners, my_first, 0), axis=1)
        tok_cap = BLOCK * owner_blocks(tok_owner)

        def cold_round(carry):
            step, cold, _ = carry
            want = owner_first[:, None] + step * my_cap + slot
            ids = jnp.sum(jnp.where(want[:, :, None] == pos, ids_all[:, None, :], 0), axis=2) - base
            pick = (ids.reshape(-1, 1) == jnp.arange(HOT_ROWS, dtype=jnp.int32)).astype(jnp.bfloat16)
            rows = dot(pick, hot_own, ((1,), (0,))).astype(jnp.bfloat16)
            got, handed = cold_exchange([rows.reshape(NUM_DEV, MOST, BLOCK, width), hot_blocks], 6)
            at = tok_slot - step * tok_cap
            here = (tok_owner > 0) & (at >= 0) & (at < tok_cap)
            mine = jnp.take(got.reshape(-1, width), jnp.where(here, tok_owner * CAP + at, 0), axis=0)
            return step + 1, jnp.where(here[:, None], mine, cold), handed

        hot_blocks = hot_own.reshape(NUM_DEV, HOT_ROWS // NUM_DEV, width)
        carry = cold_round((jnp.int32(0), jnp.zeros((n_tok, width), jnp.bfloat16), None))
        _, cold, handed = lax.while_loop(lambda carry: carry[0] < rounds, cold_round, carry)

        shards = [w.astype(jnp.bfloat16) for w in (wq_shard, wk_shard, wv_shard)]
        wq_full, wk_full, wv_full, hot = all_gather_blocks([*shards, handed[0]], GATHER_PLAN, 1)

        hot_sel = ((tok[:, None] == jnp.arange(HOT_ROWS, dtype=jnp.int32)) & (tok[:, None] < vocab_local)).astype(jnp.bfloat16)
        x_rows = dot(hot_sel, hot, ((1,), (0,))) + cold.astype(jnp.float32)
        inv_rms, h_rows, normed = norm_forward(x_rows, gain_full)
        dq, dk, dv = d_query[0], d_key[0], d_value[0]
        normed_pair = jnp.concatenate([normed, partner(normed)], axis=0)
        d_w = [dot(normed_pair, paired(d), ((0,), (0,))) for d in (dq, dk, dv)]
        query_proj, key_proj, value_proj = [dot(normed, w, ((1,), (0,))).astype(jnp.bfloat16)[None]
                                            for w in (wq_full, wk_full, wv_full)]
        d_normed = (dot(dq, wq_full, ((1,), (1,))) + dot(dk, wk_full, ((1,), (1,))) + dot(dv, wv_full, ((1,), (1,))))
        gain_part = jnp.sum(d_normed * h_rows, axis=0)
        u_rows = d_normed * gain_full
        d_x = inv_rms * (u_rows - h_rows * jnp.mean(u_rows * h_rows, axis=-1, keepdims=True))

        pair_ids = jnp.concatenate([tok, partner(tok)])
        pair_sel = ((pair_ids[:, None] == jnp.arange(HOT_ROWS, dtype=jnp.int32)) & (pair_ids[:, None] < vocab_local)).astype(jnp.float32)
        hot_part = dot(pair_sel, paired(d_x), ((0,), (0,)), lax.Precision.HIGHEST)
        def owner_rows(step):
            want = my_first[:, None] + step * caps[:, None] + slot
            src = jnp.sum(jnp.where(want[:, :, None] == rank, pos, 0), axis=2)
            return jnp.take(d_x, src.reshape(-1), axis=0).reshape(NUM_DEV, MOST, BLOCK, width)

        def add_round(step, total, got, fresh):
            left = jnp.clip(owner_count - step * my_cap, 0, my_cap)
            return add_rows(fresh, vocab_local, ids_all, owner_first + step * my_cap, left, base, total, got)

        d_w_query, d_w_key, d_w_value, hot_sum, cold_got = reduce_scatter_blocks(
            [*d_w, hot_part], owner_rows(0), REDUCE_PLAN, (3,), 2)

        gain_blocks = jnp.pad(gain_part.reshape(NUM_DEV, 1, -1), ((0, 0), (0, 0), (0, 128 - gain_rows)))
        d_norm_gain = jnp.sum(exchange([gain_blocks], 5)[0], axis=(0, 1))[:gain_rows]
        def more_rows(carry):
            step, total = carry
            return step + 1, add_round(step, total, cold_exchange([owner_rows(step)], 7)[0], False)

        _, d_embed = lax.while_loop(lambda carry: carry[0] < rounds, more_rows,
                                    (jnp.int32(1), add_round(jnp.int32(0), hot_sum, cold_got, True)))
        return (query_proj, key_proj, value_proj, d_embed, d_norm_gain, d_w_query, d_w_key, d_w_value)

    row_spec = P(AXIS_NAME, None)
    act_spec = P(AXIS_NAME, None, None)
    vec_spec = P(AXIS_NAME)
    return jax.shard_map(local_step, mesh=mesh,
                         in_specs=(row_spec, row_spec, vec_spec, row_spec, row_spec, row_spec, act_spec, act_spec, act_spec),
                         out_specs=(act_spec, act_spec, act_spec, row_spec, vec_spec, row_spec, row_spec, row_spec),
                         check_vma=False)
```
